128 devices in a mesh: sub: 8 (over z, core), ma: 16 (over y, x).
Axes of the slice: x: 4, y: 4, z: 4, core: 2. Of those that a mesh axis runs over, the one named last changes fastest.
Arguments:
- forcing: float32 [2, 512, 2, 128, 512], P(None, 'sub', None, 'ma'), may hold values from -24 to 24
- slot_wavenumber: int32 [128], P('ma'), may hold values from 0 to 511, as said below
- inverse: float32 [8, 2, 64, 64, 512], P('sub'), may hold values from -2 to 2
- edge_weights: float32 [8, 2, 64], P('sub'), may hold values from -2908 to 2908, as said below
Outputs:
- transform_field: float32 [2, 512, 2, 128, 512], P(None, ('sub', 'ma'))
The draws below stay inside these ranges and needn't reach their ends.
Inputs may be any that keep to these rules, and one draw needn't show every extreme that they name: `slot_wavenumber`: each device's slots hold 4 pairs: slots 2j and 2j + 1 carry a wavenumber m below 256 and 511 - m, in that order; no wavenumber appears twice. `edge_weights`: together with inverse it makes every row of the interface system strictly diagonally dominant with a positive diagonal.
All inputs are finite; a program needn't handle non-finite values.
Results may differ from the reference program's by a relative error of at most 0.0003.
Values sent between devices are 32-bit elements; how exact they have to be, the bound alone decides.
No kernel may reach another device: no remote copies, remote signals or barrier semaphores. Data moves between devices by JAX's collectives and lax.ppermute only.
A program may use at most 192 MiB of HBM per device.

```python
import math
import jax
import jax.numpy as jnp
from jax import lax

P_SIZE = 64
L = 512
FIELDS = 2
NSUB = 8
MTOT = 128
NR = 512


def shell_radius(key):
    widths = jax.random.uniform(jax.random.fold_in(key, 11), (NSUB,), jnp.float32, 1.0, 2.0)
    widths = 0.65 * widths / jnp.sum(widths)
    starts = 0.35 + jnp.cumsum(widths) - widths
    spacing = jnp.arange(P_SIZE, dtype=jnp.float32) / (P_SIZE - 1)
    return (starts[:, None] + widths[:, None] * spacing[None, :], widths)


def draw_slot_wavenumber(key, part):
    halfway = L // 2
    chosen = jax.random.permutation(jax.random.fold_in(key, 21), halfway)[:MTOT // 2]
    paired = jnp.stack([chosen, L - 1 - chosen], axis=1).reshape(MTOT)
    return paired.astype(jnp.int32)


def draw_edge_weights(key, part):
    radius, widths = shell_radius(key)
    step_size = widths / (P_SIZE - 1)
    lower_row = jnp.zeros((NSUB, P_SIZE), jnp.float32)
    lower_row = lower_row.at[:, 0].set(-1.5 / step_size).at[:, 1].set(2.0 / step_size).at[:, 2].set(-0.5 / step_size)
    upper_row = jnp.zeros((NSUB, P_SIZE), jnp.float32)
    upper_row = upper_row.at[:, P_SIZE - 1].set(1.5 / step_size).at[:, P_SIZE - 2].set(-2.0 / step_size).at[:, P_SIZE - 3].set(0.5 / step_size)
    return jnp.stack([lower_row, upper_row], axis=1)


def draw_inverse(key, part):
    radius, widths = shell_radius(key)
    field_scale = jnp.exp(jax.random.uniform(jax.random.fold_in(key, 12), (FIELDS,), jnp.float32, math.log(0.05), math.log(0.5)))
    degree_scale = jnp.exp(jax.random.uniform(jax.random.fold_in(key, 13), (FIELDS, L), jnp.float32, 0.0, math.log(3.0)))
    strength = (field_scale[:, None] * degree_scale)[None, :, :, None]
    degree = jnp.arange(L, dtype=jnp.float32)
    angular = degree * (degree + 1.0)
    inner = radius[:, 1:-1]
    below_gap = radius[:, 1:-1] - radius[:, :-2]
    above_gap = radius[:, 2:] - radius[:, 1:-1]
    spans = below_gap + above_gap
    sub_coef = 2.0 / (below_gap * spans) - 2.0 / (inner * spans)
    sup_coef = 2.0 / (above_gap * spans) + 2.0 / (inner * spans)
    mid_coef = 2.0 / (below_gap * above_gap)
    lower_band = -strength * sub_coef[:, None, None, :]
    upper_band = -strength * sup_coef[:, None, None, :]
    main_band = 1.0 + strength * (mid_coef[:, None, None, :] + angular[None, None, :, None] / (inner[:, None, None, :] * inner[:, None, None, :]))
    edges = ((0, 0), (0, 0), (0, 0), (1, 1))
    lower_band = jnp.pad(lower_band, edges)
    upper_band = jnp.pad(upper_band, edges)
    main_band = jnp.pad(main_band, edges, constant_values=1.0)
    bands = (jnp.moveaxis(lower_band, -1, 0), jnp.moveaxis(main_band, -1, 0), jnp.moveaxis(upper_band, -1, 0), jnp.eye(P_SIZE, dtype=jnp.float32))

    def forward(state_pair, inputs):
        prior_ratio, prior_value = state_pair
        sub_entry, main_entry, sup_entry, unit_row = inputs
        pivot_value = main_entry - sub_entry * prior_ratio
        ratio_next = sup_entry / pivot_value
        value_next = (unit_row[None, None, None, :] - sub_entry[..., None] * prior_value) / pivot_value[..., None]
        return ((ratio_next, value_next), (ratio_next, value_next))
    initial = (jnp.zeros((NSUB, FIELDS, L), jnp.float32), jnp.zeros((NSUB, FIELDS, L, P_SIZE), jnp.float32))
    _, (ratios, values) = lax.scan(forward, initial, bands)

    def backward(later_value, inputs):
        ratio_here, value_here = inputs
        current = value_here - ratio_here[..., None] * later_value
        return (current, current)
    _, solved = lax.scan(backward, jnp.zeros((NSUB, FIELDS, L, P_SIZE), jnp.float32), (ratios, values), reverse=True)
    position = jnp.arange(P_SIZE)
    interior = ((position > 0) & (position < P_SIZE - 1)).astype(jnp.float32)
    noise = jax.random.truncated_normal(jax.random.fold_in(key, 14), -3.0, 3.0, (NSUB, FIELDS, P_SIZE, P_SIZE, L), jnp.float32)
    inner_mask = (interior[:, None] * interior[None, :])[None, None, :, :, None]
    mixing = jnp.eye(P_SIZE, dtype=jnp.float32)[None, None, :, :, None] + 0.5 * noise / math.sqrt(P_SIZE - 2) * inner_mask
    return jnp.einsum('isflk,sfkjl->sfijl', solved, mixing, precision=lax.Precision.HIGHEST)


def block_levels(rng, dims, split, smallest, largest):
    def one(dim, blocks):
        draws = jax.random.uniform(jax.random.fold_in(jax.random.fold_in(rng, 6), dim), (blocks,), jnp.float32, smallest / len(split), largest / len(split))
        return jnp.repeat(jnp.exp(draws), dims[dim] // blocks).reshape((-1,) + (1,) * (len(dims) - dim - 1))

    loudness = one(*split[0])
    for cut in split[1:]:
        loudness = loudness * one(*cut)
    return loudness


def scatter_about(key, shape, scale, most, split=(), held_as=jnp.bfloat16):
    drawn = scale * jax.random.normal(key, shape, jnp.float32)
    if split:
        drawn = drawn * block_levels(key, shape, split, -0.22, 0.18)
    return jnp.clip(drawn, -most, most).astype(held_as)


def setup_inputs(seed: int = 0) -> dict:
    arg_keys = jax.random.split(jax.random.key(seed), 5)
    forcing = scatter_about(arg_keys[0], (FIELDS, NR, 2, MTOT, L), 4.0, 24.0, ((1, 8), (3, 16)), jnp.float32)
    slot_wavenumber = draw_slot_wavenumber(jax.random.fold_in(arg_keys[4], 71), 0)
    inverse = draw_inverse(jax.random.fold_in(arg_keys[4], 71), 0)
    edge_weights = draw_edge_weights(jax.random.fold_in(arg_keys[4], 71), 0)
    return {"forcing": forcing, "slot_wavenumber": slot_wavenumber, "inverse": inverse, "edge_weights": edge_weights}


HIGH = lax.Precision.HIGHEST


def local_solve(pair):
    block_inverse, block_source = pair
    return jnp.einsum('fpql,fqcml->fpcml', block_inverse, block_source, precision=HIGH)


def reference(forcing, slot_wavenumber, inverse, edge_weights):
    degree = jnp.arange(L, dtype=jnp.int32)
    kept_modes = (degree[None, :] >= slot_wavenumber[:, None]).astype(jnp.float32)
    position = jnp.arange(P_SIZE, dtype=jnp.int32)
    interior = ((position > 0) & (position < P_SIZE - 1)).astype(jnp.float32)
    source = forcing.reshape(FIELDS, NSUB, P_SIZE, 2, MTOT, L)
    source = source * kept_modes[None, None, None, None, :, :] * interior[None, None, :, None, None, None]
    source = jnp.transpose(source, (1, 0, 2, 3, 4, 5))
    particular = lax.map(local_solve, (inverse, source))
    low_row = edge_weights[:, 0, :]
    top_row = edge_weights[:, 1, :]
    low_slope = jnp.einsum('sp,sfpcml->sfcml', low_row, particular, precision=HIGH)
    top_slope = jnp.einsum('sp,sfpcml->sfcml', top_row, particular, precision=HIGH)
    lower_unit = inverse[:, :, :, 0, :]
    upper_unit = inverse[:, :, :, P_SIZE - 1, :]
    low_lower = jnp.einsum('sp,sfpl->sfl', low_row, lower_unit, precision=HIGH)
    low_upper = jnp.einsum('sp,sfpl->sfl', low_row, upper_unit, precision=HIGH)
    top_lower = jnp.einsum('sp,sfpl->sfl', top_row, lower_unit, precision=HIGH)
    top_upper = jnp.einsum('sp,sfpl->sfl', top_row, upper_unit, precision=HIGH)
    ratio_now = jnp.zeros((FIELDS, L), jnp.float32)
    reduced = jnp.zeros((FIELDS, 2, MTOT, L), jnp.float32)
    ratio_list = []
    reduced_list = []
    for level in range(NSUB - 1):
        lower_coef = top_lower[level]
        middle_coef = top_upper[level] - low_lower[level + 1]
        upper_coef = -low_upper[level + 1]
        right_side = low_slope[level + 1] - top_slope[level]
        pivot_value = middle_coef - lower_coef * ratio_now
        ratio_now = upper_coef / pivot_value
        reduced = (right_side - lower_coef[:, None, None, :] * reduced) / pivot_value[:, None, None, :]
        ratio_list.append(ratio_now)
        reduced_list.append(reduced)
    later_value = jnp.zeros((FIELDS, 2, MTOT, L), jnp.float32)
    interface = [later_value] * (NSUB - 1)
    for level in range(NSUB - 2, -1, -1):
        later_value = reduced_list[level] - ratio_list[level][:, None, None, :] * later_value
        interface[level] = later_value
    boundary = jnp.zeros((FIELDS, 2, MTOT, L), jnp.float32)
    lower_value = jnp.stack([boundary] + interface)
    upper_value = jnp.stack(interface + [boundary])
    solution = particular + lower_value[:, :, None] * lower_unit[:, :, :, None, None, :]
    solution = solution + upper_value[:, :, None] * upper_unit[:, :, :, None, None, :]
    return jnp.transpose(solution, (1, 0, 2, 3, 4, 5)).reshape(FIELDS, NR, 2, MTOT, L)
```

```python
import jax
import jax.numpy as jnp
from jax import lax
from jax.experimental import pallas as pl
from jax.experimental.pallas import tpu as pltpu
from jax.sharding import PartitionSpec as P

F32 = jnp.float32
POINTS = 64
FIELDS = 2
NSUB = 8
GROUPS = 16
LANES = 128
ROWS = 8
PACK = 5
QB = 8
PB = 8
NEAR = POINTS // GROUPS
SLOPES = 2 * FIELDS * PACK
MESSAGE = SLOPES + 4
SENT = FIELDS * NEAR * 4 + 1


def lane_iota():
    return lax.broadcasted_iota(jnp.int32, (ROWS, LANES), 1)


def row_iota():
    return lax.broadcasted_iota(jnp.int32, (ROWS, LANES), 0)


def pair_wavenumber(slot_ref):
    pair = row_iota() // 2
    m = jnp.full((ROWS, LANES), slot_ref[0], jnp.int32)
    for j in range(1, 4):
        m = jnp.where(pair == j, slot_ref[2 * j], m)
    return m


def down(x):
    return pltpu.roll(x, 1, 0)


def up(x):
    return pltpu.roll(x, ROWS - 1, 0)


def slope_kernel(slot_ref, weight_ref, inv_ref, src_ref, packed_ref, msg_ref, e_ref):
    f = pl.program_id(0)
    block = pl.program_id(1)
    m = pair_wavenumber(slot_ref)
    lane = lane_iota()
    row = row_iota()
    even = row % 2 == 0
    small = m < LANES
    keep1 = lane + LANES >= m
    keep3 = lane + 3 * LANES >= jnp.where(even, m, 511 - m)
    keep_mix = lane >= jnp.where(small, m, 255 - m)

    def gather_rows(p, carry):
        out = []
        low = weight_ref[0, 0, p]
        top = weight_ref[0, 1, p]
        for b in range(4):
            tile = inv_ref[0, p, :, b * LANES:(b + 1) * LANES]
            out.append(carry[2 * b] + low * tile)
            out.append(carry[2 * b + 1] + top * tile)
        return tuple(out)

    zero = jnp.zeros((QB, LANES), F32)
    rows = lax.fori_loop(0, POINTS, gather_rows, (zero,) * 8, unroll=8)
    for b in range(4):
        e_ref[0, b] = rows[2 * b]
        e_ref[1, b] = rows[2 * b + 1]

    @pl.when(block == 0)
    def _():
        for r in range(2):
            for v in range(PACK):
                msg_ref[(r * FIELDS + f) * PACK + v] = jnp.zeros((ROWS, LANES), F32)
            for b in range(4):
                msg_ref[SLOPES + b, pl.ds(r * 4 + f * 2, 1), :] = e_ref[r, b, 0:1, :]

    @pl.when(block == POINTS // QB - 1)
    def _():
        for r in range(2):
            for b in range(4):
                msg_ref[SLOPES + b, pl.ds(r * 4 + f * 2 + 1, 1), :] = e_ref[r, b, QB - 1:QB, :]

    sums = [[msg_ref[(r * FIELDS + f) * PACK + v] for v in range(PACK)] for r in range(2)]
    for q in range(QB):
        point = block * QB + q
        inside = jnp.logical_and(point > 0, point < POINTS - 1).astype(F32)
        s = [[src_ref[0, q, c, :, b * LANES:(b + 1) * LANES] for b in range(4)] for c in range(2)]
        first = jnp.where(even, s[0][0], down(s[1][0]))
        late = jnp.where(even, up(s[0][2]), s[1][2])
        vectors = [
            jnp.where(keep1, jnp.where(even, s[0][1], down(s[1][1])), 0.0),
            jnp.where(even, s[0][2], down(s[1][2])),
            jnp.where(keep3, s[0][3], 0.0),
            jnp.where(keep3, s[1][3], 0.0),
            jnp.where(keep_mix, jnp.where(small, first, late), 0.0),
        ]
        vectors = [v * inside for v in vectors]
        for v in range(PACK):
            packed_ref[0, q, v] = vectors[v]
        for r in range(2):
            e = [e_ref[r, b, pl.ds(q, ROWS, stride=0), :] for b in range(4)]
            e = [e[1], e[2], e[3], e[3], jnp.where(small, e[0], e[2])]
            for v in range(PACK):
                sums[r][v] = sums[r][v] + e[v] * vectors[v]
    for r in range(2):
        for v in range(PACK):
            msg_ref[(r * FIELDS + f) * PACK + v] = sums[r][v]


def slopes(slot, weights, inverse, forcing):
    return pl.pallas_call(
        slope_kernel,
        grid=(FIELDS, POINTS // QB),
        in_specs=[
            pl.BlockSpec(memory_space=pltpu.SMEM),
            pl.BlockSpec(memory_space=pltpu.SMEM),
            pl.BlockSpec((1, POINTS, QB, 512), lambda f, q: (f, 0, q, 0)),
            pl.BlockSpec((1, QB, 2, ROWS, 512), lambda f, q: (f, q, 0, 0, 0)),
        ],
        out_specs=[
            pl.BlockSpec((1, QB, PACK, ROWS, LANES), lambda f, q: (f, q, 0, 0, 0)),
            pl.BlockSpec((MESSAGE, ROWS, LANES), lambda f, q: (0, 0, 0)),
        ],
        out_shape=[
            jax.ShapeDtypeStruct((FIELDS, POINTS, PACK, ROWS, LANES), F32),
            jax.ShapeDtypeStruct((MESSAGE, ROWS, LANES), F32),
        ],
        scratch_shapes=[pltpu.VMEM((2, 4, QB, LANES), F32)],
        compiler_params=pltpu.CompilerParams(dimension_semantics=("arbitrary", "arbitrary")),
        cost_estimate=pl.CostEstimate(flops=20_000_000, bytes_accessed=24_000_000, transcendentals=0),
        name="slopes",
    )(slot, weights, inverse, forcing)


def solve_kernel(slot_ref, inv_ref, src_ref, part_ref, edge_ref):
    small = pair_wavenumber(slot_ref) < LANES

    def unit(p, block, r, b):
        line = inv_ref[0, p, block, r:r + 1, b * LANES:(b + 1) * LANES]
        return jnp.broadcast_to(line, (ROWS, LANES))

    def odd_pass(block, sums):
        sums = list(sums)
        for r in range(ROWS):
            s = [src_ref[0, block, r, v] for v in (0, 2, 3)]
            for p in range(PB):
                one = unit(p, block, r, 1)
                three = unit(p, block, r, 3)
                sums[3 * p] = sums[3 * p] + one * s[0]
                sums[3 * p + 1] = sums[3 * p + 1] + three * s[1]
                sums[3 * p + 2] = sums[3 * p + 2] + three * s[2]
        return tuple(sums)

    def even_pass(block, sums):
        sums = list(sums)
        for r in range(ROWS):
            s = [src_ref[0, block, r, v] for v in (1, 4)]
            for p in range(PB):
                none = unit(p, block, r, 0)
                two = unit(p, block, r, 2)
                sums[2 * p] = sums[2 * p] + two * s[0]
                sums[2 * p + 1] = sums[2 * p + 1] + jnp.where(small, none, two) * s[1]
        return tuple(sums)

    zero = jnp.zeros((ROWS, LANES), F32)
    sums = lax.fori_loop(0, POINTS // ROWS, odd_pass, (zero,) * (3 * PB))
    for p in range(PB):
        part_ref[0, p, 0] = sums[3 * p]
        part_ref[0, p, 2] = sums[3 * p + 1]
        part_ref[0, p, 3] = sums[3 * p + 2]
    sums = lax.fori_loop(0, POINTS // ROWS, even_pass, (zero,) * (2 * PB))
    for p in range(PB):
        part_ref[0, p, 1] = sums[2 * p]
        part_ref[0, p, 4] = sums[2 * p + 1]
        for b in range(4):
            lanes = slice(b * LANES, (b + 1) * LANES)
            edge_ref[0, p, 2 * b:2 * b + 1, :] = inv_ref[0, p, 0, 0:1, lanes]
            edge_ref[0, p, 2 * b + 1:2 * b + 2, :] = inv_ref[0, p, POINTS // ROWS - 1, ROWS - 1:ROWS, lanes]


def particular(slot, inverse, packed):
    return pl.pallas_call(
        solve_kernel,
        grid=(FIELDS, POINTS // PB),
        in_specs=[
            pl.BlockSpec(memory_space=pltpu.SMEM),
            pl.BlockSpec((1, PB, POINTS // ROWS, ROWS, 512), lambda f, p: (f, p, 0, 0, 0)),
            pl.BlockSpec((1, POINTS // ROWS, ROWS, PACK, ROWS, LANES), lambda f, p: (f, 0, 0, 0, 0, 0)),
        ],
        out_specs=[
            pl.BlockSpec((1, PB, PACK, ROWS, LANES), lambda f, p: (f, p, 0, 0, 0)),
            pl.BlockSpec((1, PB, ROWS, LANES), lambda f, p: (f, p, 0, 0)),
        ],
        out_shape=[
            jax.ShapeDtypeStruct((FIELDS, POINTS, PACK, ROWS, LANES), F32),
            jax.ShapeDtypeStruct((FIELDS, POINTS, ROWS, LANES), F32),
        ],
        compiler_params=pltpu.CompilerParams(dimension_semantics=("arbitrary", "arbitrary")),
        cost_estimate=pl.CostEstimate(flops=90_000_000, bytes_accessed=24_000_000, transcendentals=0),
        name="particular",
    )(
        slot,
        inverse.reshape(FIELDS, POINTS, POINTS // ROWS, ROWS, 512),
        packed.reshape(FIELDS, POINTS // ROWS, ROWS, PACK, ROWS, LANES),
    )


DEST = 4


def pack_kernel(slot_ref, *refs):
    blocks = refs[:NSUB]
    part_ref, edge_ref, out_ref, all_ref, u_ref = refs[NSUB:]
    sub = lax.axis_index("sub")
    m = pair_wavenumber(slot_ref)
    lane = lane_iota()
    row = row_iota()
    even = row % 2 == 0
    small = m < LANES

    @pl.when(pl.program_id(0) == 0)
    def _():
        for k in range(NSUB):
            place = lax.rem(sub + (NSUB - k), NSUB)
            for i in range(MESSAGE):
                all_ref[place, i] = blocks[k][i]
        zero = jnp.zeros((ROWS, LANES), F32)
        for f in range(FIELDS):
            for v in range(PACK):
                u_ref[0, f, v] = zero
                u_ref[NSUB, f, v] = zero

            def coefficient(t, r, k, b):
                return all_ref[t, SLOPES + b, pl.ds(r * 4 + f * 2 + k, ROWS, stride=0), :]

            ratio = [zero] * PACK
            reduced = [zero] * PACK
            ratios = []
            reduceds = []
            for level in range(NSUB - 1):
                factors = []
                for b in range(4):
                    lower = coefficient(level, 1, 0, b)
                    middle = coefficient(level, 1, 1, b) - coefficient(level + 1, 0, 0, b)
                    upper = -coefficient(level + 1, 0, 1, b)
                    factors.append((lower, middle, upper))
                mixed = tuple(jnp.where(small, x, y) for x, y in zip(factors[0], factors[2]))
                new_ratio, new_reduced = [None] * PACK, [None] * PACK
                for v, (lower, middle, upper) in enumerate((factors[1], factors[2], factors[3], factors[3], mixed)):
                    right = (
                        all_ref[level + 1, f * PACK + v]
                        - all_ref[level, (FIELDS + f) * PACK + v]
                    )
                    if v == 3:
                        inverted = last
                    else:
                        inverted = 1.0 / (middle - lower * ratio[v])
                    last = inverted
                    new_ratio[v] = upper * inverted
                    new_reduced[v] = (right - lower * reduced[v]) * inverted
                ratio, reduced = new_ratio, new_reduced
                ratios.append(ratio)
                reduceds.append(reduced)
            later = [zero] * PACK
            for level in range(NSUB - 2, -1, -1):
                later = [reduceds[level][v] - ratios[level][v] * later[v] for v in range(PACK)]
                for v in range(PACK):
                    u_ref[level + 1, f, v] = later[v]

    shift = jnp.where(small, m, m - LANES)
    turn = (lane - shift + LANES) % LANES
    below = lane < shift
    extra_at = LANES - 1 - shift
    for d in range(DEST):
        extra = jnp.where(lane == FIELDS * NEAR, m.astype(F32), 0.0)
        for f in range(FIELDS):
            u_low = [u_ref[sub, f, v] for v in range(PACK)]
            u_top = [u_ref[sub + 1, f, v] for v in range(PACK)]
            for k in range(NEAR):
                p = d * NEAR + k
                low = [edge_ref[f, p, pl.ds(2 * b, ROWS, stride=0), :] for b in range(4)]
                top = [edge_ref[f, p, pl.ds(2 * b + 1, ROWS, stride=0), :] for b in range(4)]
                low = [low[1], low[2], low[3], low[3], jnp.where(small, low[0], low[2])]
                top = [top[1], top[2], top[3], top[3], jnp.where(small, top[0], top[2])]
                x = [
                    part_ref[f, p, v] + u_low[v] * low[v] + u_top[v] * top[v] for v in range(PACK)
                ]
                low3 = jnp.where(even, x[2], down(x[3]))
                high3 = jnp.where(even, up(x[2]), x[3])
                mix = x[4]
                high3_t = jnp.take_along_axis(high3, turn, axis=1)
                mix_t = jnp.take_along_axis(mix, turn, axis=1)
                at = (f * NEAR + k) * 4
                out_ref[d, at] = jnp.where(
                    small,
                    jnp.where(below, high3_t, mix),
                    jnp.where(below, mix_t, high3_t),
                )
                out_ref[d, at + 1] = jnp.where(jnp.logical_and(below, jnp.logical_not(small)), high3_t, x[0])
                out_ref[d, at + 2] = x[1]
                out_ref[d, at + 3] = low3
                single = jnp.take_along_axis(jnp.where(small, high3, mix), extra_at, axis=1)
                extra = jnp.where(lane == f * NEAR + k, single, extra)
        out_ref[d, SENT - 1] = extra


def pack(slot, blocks, part, edges):
    return pl.pallas_call(
        pack_kernel,
        grid=(GROUPS // DEST,),
        in_specs=[pl.BlockSpec(memory_space=pltpu.SMEM)]
        + [pl.BlockSpec((MESSAGE, ROWS, LANES), lambda d: (0, 0, 0))] * NSUB
        + [
            pl.BlockSpec((FIELDS, DEST * NEAR, PACK, ROWS, LANES), lambda d: (0, d, 0, 0, 0)),
            pl.BlockSpec((FIELDS, DEST * NEAR, ROWS, LANES), lambda d: (0, d, 0, 0)),
        ],
        out_specs=pl.BlockSpec((DEST, SENT, ROWS, LANES), lambda d: (d, 0, 0, 0)),
        out_shape=jax.ShapeDtypeStruct((GROUPS, SENT, ROWS, LANES), F32),
        scratch_shapes=[
            pltpu.VMEM((NSUB, MESSAGE, ROWS, LANES), F32),
            pltpu.VMEM((NSUB + 1, FIELDS, PACK, ROWS, LANES), F32),
        ],
        compiler_params=pltpu.CompilerParams(dimension_semantics=("arbitrary",)),
        name="pack",
    )(slot, *blocks, part, edges)


FROM = 4


def unpack_kernel(in_ref, out_ref):
    lane = lane_iota()
    even = row_iota() % 2 == 0
    zero = jnp.zeros((ROWS, LANES), F32)
    for g in range(FROM):
        extras = in_ref[g, SENT - 1]
        m = jnp.take_along_axis(extras, jnp.full((ROWS, LANES), FIELDS * NEAR, jnp.int32), axis=1).astype(jnp.int32)
        small = m < LANES
        shift = jnp.where(small, m, m - LANES)
        back = (lane + shift) % LANES
        after = lane >= LANES - shift
        exact = lane == LANES - 1 - shift
        own0 = lane >= m
        own1 = lane + LANES >= m
        at_rows = pl.ds(g * ROWS, ROWS)
        for f in range(FIELDS):
            for k in range(NEAR):
                at = (f * NEAR + k) * 4
                s = [in_ref[g, at + b] for b in range(4)]
                single = jnp.take_along_axis(extras, jnp.full((ROWS, LANES), f * NEAR + k, jnp.int32), axis=1)
                g0 = jnp.take_along_axis(s[0], back, axis=1)
                g1 = jnp.take_along_axis(s[1], back, axis=1)
                value = jnp.where(after, g0, jnp.where(exact, single, 0.0))
                high3 = jnp.where(small, value, jnp.where(after, g1, g0))
                high2 = jnp.where(small, 0.0, value)
                low0 = jnp.where(own0, s[0], 0.0)
                low1 = jnp.where(own1, s[1], 0.0)
                lows = [low0, low1, s[2], s[3]]
                highs = [zero, zero, high2, high3]
                for b in range(4):
                    lanes = slice(b * LANES, (b + 1) * LANES)
                    high_first = highs[b] if b < 2 else down(highs[b])
                    out_ref[f, k, 0, at_rows, lanes] = jnp.where(even, lows[b], high_first)
                    out_ref[f, k, 1, at_rows, lanes] = jnp.where(even, up(lows[b]), highs[b])


def unpack(received):
    return pl.pallas_call(
        unpack_kernel,
        grid=(GROUPS // FROM,),
        in_specs=[pl.BlockSpec((FROM, SENT, ROWS, LANES), lambda g: (g, 0, 0, 0))],
        out_specs=pl.BlockSpec((FIELDS, NEAR, 2, FROM * ROWS, 512), lambda g: (0, 0, 0, g, 0)),
        out_shape=jax.ShapeDtypeStruct((FIELDS, NEAR, 2, GROUPS * ROWS, 512), F32),
        compiler_params=pltpu.CompilerParams(dimension_semantics=("arbitrary",)),
        name="unpack",
    )(received)


def body(forcing, slot_wavenumber, inverse, edge_weights):
    packed, message = slopes(slot_wavenumber, edge_weights, inverse[0], forcing)
    blocks = [message]
    for k in range(1, NSUB):
        blocks.append(lax.ppermute(message, "sub", [(i, (i + k) % NSUB) for i in range(NSUB)]))
    part, edges = particular(slot_wavenumber, inverse[0], packed)
    sent = pack(slot_wavenumber, blocks, part, edges)
    sent = sent.reshape(GROUPS, SENT * ROWS, LANES)
    received = lax.all_to_all(sent, "ma", split_axis=0, concat_axis=0, tiled=True)
    return unpack(received.reshape(GROUPS, SENT, ROWS, LANES))


def solution(mesh):
    return jax.shard_map(
        body,
        mesh=mesh,
        in_specs=(
            P(None, "sub", None, "ma", None),
            P("ma"),
            P("sub", None, None, None, None),
            P("sub", None, None),
        ),
        out_specs=P(None, ("sub", "ma"), None, None, None),
        check_vma=False,
    )
```

```python
import jax
import jax.numpy as jnp
from jax import lax
from jax.experimental import pallas as pl
from jax.experimental.pallas import tpu as pltpu
from jax.sharding import PartitionSpec as P

F32 = jnp.float32
POINTS = 64
FIELDS = 2
NSUB = 8
GROUPS = 16
LANES = 128
ROWS = 8
PACK = 5
QB = 8
PB = 8
NEAR = POINTS // GROUPS
SENT = FIELDS * NEAR * 4 + 1
MESSAGE = 2 * PACK + 2
BLOCKS = POINTS // PB


def lane_iota():
    return lax.broadcasted_iota(jnp.int32, (ROWS, LANES), 1)


def row_iota():
    return lax.broadcasted_iota(jnp.int32, (ROWS, LANES), 0)


def pair_wavenumber(slot_ref):
    pair = row_iota() // 2
    m = jnp.full((ROWS, LANES), slot_ref[0], jnp.int32)
    for j in range(1, 4):
        m = jnp.where(pair == j, slot_ref[2 * j], m)
    return m


def down(x):
    return pltpu.roll(x, 1, 0)


def up(x):
    return pltpu.roll(x, ROWS - 1, 0)


def fold(x, m, lane, even, small):
    shift = jnp.where(small, m, m - LANES)
    turn = (lane - shift + LANES) % LANES
    below = lane < shift
    low3 = jnp.where(even, x[2], down(x[3]))
    high3 = jnp.where(even, up(x[2]), x[3])
    high3_t = jnp.take_along_axis(high3, turn, axis=1)
    mix_t = jnp.take_along_axis(x[4], turn, axis=1)
    zero = jnp.where(small, jnp.where(below, high3_t, x[4]), jnp.where(below, mix_t, high3_t))
    one = jnp.where(jnp.logical_and(below, jnp.logical_not(small)), high3_t, x[0])
    last = jnp.full((ROWS, LANES), LANES - 1, jnp.int32)
    spare = jnp.take_along_axis(jnp.where(small, high3_t, mix_t), last, axis=1)
    return (zero, one, x[1], low3), spare


def column(x, k):
    return jnp.take_along_axis(x, jnp.full((ROWS, LANES), k, jnp.int32), axis=1)


def unfold(s, spare, m, lane, even, small):
    shift = jnp.where(small, m, m - LANES)
    back = (lane + shift) % LANES
    after = lane >= LANES - shift
    exact = lane == LANES - 1 - shift
    g0 = jnp.take_along_axis(s[0], back, axis=1)
    g1 = jnp.take_along_axis(s[1], back, axis=1)
    value = jnp.where(after, g0, jnp.where(exact, spare, 0.0))
    high3 = jnp.where(small, value, jnp.where(after, g1, g0))
    high2 = jnp.where(small, 0.0, value)
    low0 = jnp.where(lane >= m, s[0], 0.0)
    low1 = jnp.where(lane + LANES >= m, s[1], 0.0)
    lows = [low0, low1, s[2], s[3]]
    first = [jnp.where(even, low0, 0.0), jnp.where(even, low1, 0.0)]
    first += [jnp.where(even, s[2], down(high2)), jnp.where(even, s[3], down(high3))]
    second = [jnp.where(even, up(low0), 0.0), jnp.where(even, up(low1), 0.0)]
    second += [jnp.where(even, up(s[2]), high2), jnp.where(even, up(s[3]), high3)]
    return first, second


AHEAD = 4
CHUNKS = FIELDS * BLOCKS


def inverse_chunks(inv_hbm, inv_v, sem):
    def copy(i):
        f = i // BLOCKS
        rows = pl.ds(lax.rem(i, BLOCKS) * PB, PB)
        return pltpu.make_async_copy(inv_hbm.at[f, rows], inv_v.at[f, rows], sem.at[i])

    return copy


def next_chunk(copy, i):
    copy(i).wait()

    @pl.when(i + AHEAD < CHUNKS)
    def _():
        copy(i + AHEAD).start()


def start_all(copy, count):
    def step(i, carry):
        copy(i).start()
        return carry

    lax.fori_loop(0, count, step, 0)


def wait_all(copy, count):
    def step(i, carry):
        copy(i).wait()
        return carry

    lax.fori_loop(0, count, step, 0)


def slope_kernel(
    slot_ref, weight_ref, inv_hbm, src_hbm, packed_hbm, msg_hbm, inv_v, src_v, packed_v, e_v, msg_ref, inv_sem, src_sem, out_sem, msg_sem
):
    copy = inverse_chunks(inv_hbm, inv_v, inv_sem)
    sources = [pltpu.make_async_copy(src_hbm.at[f], src_v.at[f], src_sem.at[f]) for f in range(FIELDS)]
    results = [pltpu.make_async_copy(packed_v.at[f], packed_hbm.at[f], out_sem.at[f]) for f in range(FIELDS)]
    sources[0].start()
    start_all(copy, AHEAD)
    m = pair_wavenumber(slot_ref)
    lane = lane_iota()
    even = row_iota() % 2 == 0
    small = m < LANES
    zero = jnp.zeros((ROWS, LANES), F32)
    keep1 = lane + LANES >= m
    keep3 = lane + 3 * LANES >= jnp.where(even, m, 511 - m)
    keep_mix = lane >= jnp.where(small, m, 255 - m)
    for f in range(FIELDS):
        sources[f].wait()

        def pack_point(q, carry):
            s = [[src_v[f, q, c, :, b * LANES:(b + 1) * LANES] for b in range(4)] for c in range(2)]
            first = jnp.where(even, s[0][0], down(s[1][0]))
            late = jnp.where(even, up(s[0][2]), s[1][2])
            packed_v[f, q, 0] = jnp.where(keep1, jnp.where(even, s[0][1], down(s[1][1])), 0.0)
            packed_v[f, q, 1] = jnp.where(even, s[0][2], down(s[1][2]))
            packed_v[f, q, 2] = jnp.where(keep3, s[0][3], 0.0)
            packed_v[f, q, 3] = jnp.where(keep3, s[1][3], 0.0)
            packed_v[f, q, 4] = jnp.where(keep_mix, jnp.where(small, first, late), 0.0)
            return carry

        lax.fori_loop(1, POINTS - 1, pack_point, 0, unroll=2)
        for q in (0, POINTS - 1):
            for v in range(PACK):
                packed_v[f, q, v] = zero
        results[f].start()
        if f + 1 < FIELDS:
            sources[f + 1].start()

        for r in range(2):
            for qb in range(POINTS // ROWS):
                for b in range(4):
                    e_v[r, qb, b] = zero

        def weigh(block, carry):
            next_chunk(copy, f * BLOCKS + block)
            weights = [[weight_ref[0, r, block * PB + p] for p in range(PB)] for r in range(2)]

            def tile_row(qb, carry):
                for b in range(4):
                    low, top = e_v[0, qb, b], e_v[1, qb, b]
                    for p in range(PB):
                        tile = inv_v[f, block * PB + p, qb, :, b * LANES:(b + 1) * LANES]
                        low = low + weights[0][p] * tile
                        top = top + weights[1][p] * tile
                    e_v[0, qb, b] = low
                    e_v[1, qb, b] = top
                return carry

            return lax.fori_loop(0, POINTS // ROWS, tile_row, carry)

        lax.fori_loop(0, BLOCKS, weigh, 0)

        def accumulate(qb, sums):
            sums = list(sums)
            for row in range(ROWS):
                x = [packed_v[f, qb * ROWS + row, v] for v in range(PACK)]
                for r in range(2):
                    e = [jnp.broadcast_to(e_v[r, qb, b, row:row + 1, :], (ROWS, LANES)) for b in range(4)]
                    e = [e[1], e[2], e[3], e[3], jnp.where(small, e[0], e[2])]
                    for v in range(PACK):
                        sums[r * PACK + v] = sums[r * PACK + v] + e[v] * x[v]
            return tuple(sums)

        sums = lax.fori_loop(0, POINTS // ROWS, accumulate, (zero,) * (2 * PACK))
        for i in range(2 * PACK):
            msg_ref[f * MESSAGE + i] = sums[i]
        for r in range(2):
            for b in range(4):
                msg_ref[f * MESSAGE + 2 * PACK + r, 2 * b:2 * b + 1, :] = e_v[r, 0, b, 0:1, :]
                msg_ref[f * MESSAGE + 2 * PACK + r, 2 * b + 1:2 * b + 2, :] = (
                    e_v[r, POINTS // ROWS - 1, b, ROWS - 1:ROWS, :]
                )

    def message_copy(k):
        return pltpu.make_async_copy(msg_ref, msg_hbm.at[k], msg_sem.at[k])

    start_all(message_copy, NSUB)
    for f in range(FIELDS):
        results[f].wait()
    wait_all(message_copy, NSUB)


ANY = pl.BlockSpec(memory_space=pl.ANY)
SCALARS = pl.BlockSpec(memory_space=pltpu.SMEM)
INVERSE_V = pltpu.VMEM((FIELDS, POINTS, POINTS // ROWS, ROWS, 512), F32)
PACKED_V = pltpu.VMEM((FIELDS, POINTS, PACK, ROWS, LANES), F32)
EDGE_V = pltpu.VMEM((FIELDS, POINTS, ROWS, LANES), F32)


def dma(*shape):
    return pltpu.SemaphoreType.DMA(shape)


def slopes(slot, weights, inverse, forcing):
    return pl.pallas_call(
        slope_kernel,
        in_specs=[SCALARS, SCALARS, ANY, ANY],
        out_specs=[ANY, ANY],
        out_shape=[
            jax.ShapeDtypeStruct((FIELDS, POINTS, PACK, ROWS, LANES), F32),
            jax.ShapeDtypeStruct((NSUB, FIELDS * MESSAGE, ROWS, LANES), F32),
        ],
        scratch_shapes=[
            INVERSE_V,
            pltpu.VMEM((FIELDS, POINTS, 2, ROWS, 512), F32),
            pltpu.VMEM((FIELDS, POINTS, PACK, ROWS, LANES), F32),
            pltpu.VMEM((2, POINTS // ROWS, 4, ROWS, LANES), F32),
            pltpu.VMEM((FIELDS * MESSAGE, ROWS, LANES), F32),
            dma(CHUNKS),
            dma(FIELDS),
            dma(FIELDS),
            dma(NSUB),
        ],
        cost_estimate=pl.CostEstimate(flops=20_000_000, bytes_accessed=24_000_000, transcendentals=0),
        name="slopes",
    )(slot, weights, inverse, forcing)


def block_sums(f, inv_v, packed_v, block, small, odd_v):
    zero = jnp.zeros((ROWS, LANES), F32)

    def unit(p, qb, r, b):
        line = inv_v[f, block * PB + p, qb, r:r + 1, b * LANES:(b + 1) * LANES]
        return jnp.broadcast_to(line, (ROWS, LANES))

    def odd_pass(qb, sums):
        sums = list(sums)
        for r in range(ROWS):
            s = [packed_v[f, qb * ROWS + r, v] for v in (0, 2, 3)]
            for p in range(PB):
                one = unit(p, qb, r, 1)
                three = unit(p, qb, r, 3)
                sums[3 * p] = sums[3 * p] + one * s[0]
                sums[3 * p + 1] = sums[3 * p + 1] + three * s[1]
                sums[3 * p + 2] = sums[3 * p + 2] + three * s[2]
        return tuple(sums)

    def even_pass(qb, sums):
        sums = list(sums)
        for r in range(ROWS):
            s = [packed_v[f, qb * ROWS + r, v] for v in (1, 4)]
            for p in range(PB):
                none = unit(p, qb, r, 0)
                two = unit(p, qb, r, 2)
                sums[2 * p] = sums[2 * p] + two * s[0]
                sums[2 * p + 1] = sums[2 * p + 1] + jnp.where(small, none, two) * s[1]
        return tuple(sums)

    odd = lax.fori_loop(0, POINTS // ROWS, odd_pass, (zero,) * (3 * PB))
    for i in range(3 * PB):
        odd_v[i] = odd[i]
    even = lax.fori_loop(0, POINTS // ROWS, even_pass, (zero,) * (2 * PB))
    return [[odd_v[3 * p], even[2 * p], odd_v[3 * p + 1], odd_v[3 * p + 2], even[2 * p + 1]] for p in range(PB)]


def particular_kernel(
    slot_ref, inv_hbm, packed_hbm, part_hbm, edge_hbm, inv_v, packed_v, part_v, edge_v, odd_v, inv_sem, src_sem, part_sem, edge_sem
):
    copy = inverse_chunks(inv_hbm, inv_v, inv_sem)
    sources = [pltpu.make_async_copy(packed_hbm.at[f], packed_v.at[f], src_sem.at[f]) for f in range(FIELDS)]
    sources[0].start()
    start_all(copy, AHEAD)
    small = pair_wavenumber(slot_ref) < LANES

    def part_copy(i):
        f, rows = i // BLOCKS, pl.ds(lax.rem(i, BLOCKS) * PB, PB)
        return pltpu.make_async_copy(part_v.at[f, rows], part_hbm.at[f, rows], part_sem.at[i])

    edges = [pltpu.make_async_copy(edge_v.at[f], edge_hbm.at[f], edge_sem.at[f]) for f in range(FIELDS)]
    for f in range(FIELDS):
        sources[f].wait()
        if f + 1 < FIELDS:
            sources[f + 1].start()

        def step(block, carry):
            next_chunk(copy, f * BLOCKS + block)
            x = block_sums(f, inv_v, packed_v, block, small, odd_v)
            for p in range(PB):
                at = block * PB + p
                for v in range(PACK):
                    part_v[f, at, v] = x[p][v]
                for b in range(4):
                    lanes = slice(b * LANES, (b + 1) * LANES)
                    edge_v[f, at, 2 * b:2 * b + 1, :] = inv_v[f, at, 0, 0:1, lanes]
                    edge_v[f, at, 2 * b + 1:2 * b + 2, :] = inv_v[f, at, POINTS // ROWS - 1, ROWS - 1:ROWS, lanes]
            part_copy(f * BLOCKS + block).start()
            return carry

        lax.fori_loop(0, BLOCKS, step, 0)
        edges[f].start()
    wait_all(part_copy, CHUNKS)
    for edge in edges:
        edge.wait()


def particular(slot, inverse, packed):
    return pl.pallas_call(
        particular_kernel,
        in_specs=[SCALARS, ANY, ANY],
        out_specs=[ANY, ANY],
        out_shape=[
            jax.ShapeDtypeStruct((FIELDS, POINTS, PACK, ROWS, LANES), F32),
            jax.ShapeDtypeStruct((FIELDS, POINTS, ROWS, LANES), F32),
        ],
        scratch_shapes=[
            INVERSE_V,
            PACKED_V,
            PACKED_V,
            EDGE_V,
            pltpu.VMEM((3 * PB, ROWS, LANES), F32),
            dma(CHUNKS),
            dma(FIELDS),
            dma(CHUNKS),
            dma(FIELDS),
        ],
        cost_estimate=pl.CostEstimate(flops=90_000_000, bytes_accessed=24_000_000, transcendentals=0),
        name="particular",
    )(slot, inverse, packed)


def solve_interface(f, all_v, u_v, small):
    base = f * MESSAGE
    zero = jnp.zeros((ROWS, LANES), F32)
    for v in range(PACK):
        u_v[0, f, v] = zero
        u_v[NSUB, f, v] = zero

    def coefficient(t, r, k, b):
        return all_v[t, base + 2 * PACK + r, pl.ds(2 * b + k, ROWS, stride=0), :]

    ratio = [zero] * PACK
    reduced = [zero] * PACK
    ratios = []
    reduceds = []
    for level in range(NSUB - 1):
        factors = []
        for b in range(4):
            lower = coefficient(level, 1, 0, b)
            middle = coefficient(level, 1, 1, b) - coefficient(level + 1, 0, 0, b)
            upper = -coefficient(level + 1, 0, 1, b)
            factors.append((lower, middle, upper))
        mixed = tuple(jnp.where(small, x, y) for x, y in zip(factors[0], factors[2]))
        new_ratio, new_reduced = [None] * PACK, [None] * PACK
        for v, (lower, middle, upper) in enumerate((factors[1], factors[2], factors[3], factors[3], mixed)):
            right = all_v[level + 1, base + v] - all_v[level, base + PACK + v]
            inverted = last if v == 3 else 1.0 / (middle - lower * ratio[v])
            last = inverted
            new_ratio[v] = upper * inverted
            new_reduced[v] = (right - lower * reduced[v]) * inverted
        ratio, reduced = new_ratio, new_reduced
        ratios.append(ratio)
        reduceds.append(reduced)
    later = [zero] * PACK
    for level in range(NSUB - 2, -1, -1):
        later = [reduceds[level][v] - ratios[level][v] * later[v] for v in range(PACK)]
        for v in range(PACK):
            u_v[level + 1, f, v] = later[v]


PER = PB // NEAR


def pack_kernel(
    slot_ref, all_hbm, part_hbm, edge_hbm, out_hbm, all_v, u_v, part_v, edge_v, out_v, all_sem, part_sem, edge_sem, out_sem
):
    messages = pltpu.make_async_copy(all_hbm, all_v, all_sem)
    messages.start()
    edges = pltpu.make_async_copy(edge_hbm, edge_v, edge_sem)
    edges.start()

    def part_copy(i):
        rows = pl.ds(i * PB, PB)
        return pltpu.make_async_copy(part_hbm.at[:, rows], part_v.at[:, rows], part_sem.at[i])

    start_all(part_copy, BLOCKS)
    m = pair_wavenumber(slot_ref)
    lane = lane_iota()
    even = row_iota() % 2 == 0
    small = m < LANES
    messages.wait()
    for f in range(FIELDS):
        solve_interface(f, all_v, u_v, small)
    edges.wait()
    sub = lax.axis_index("sub")

    def out_copy(i):
        rows = pl.ds(i * PER, PER)
        return pltpu.make_async_copy(out_v.at[rows], out_hbm.at[rows], out_sem.at[i])

    def step(block, carry):
        part_copy(block).wait()
        for d in range(PER):
            dest = block * PER + d
            extra = jnp.where(lane == FIELDS * NEAR, m.astype(F32), 0.0)
            for f in range(FIELDS):
                u_low = [u_v[sub, f, v] for v in range(PACK)]
                u_top = [u_v[sub + 1, f, v] for v in range(PACK)]
                for k in range(NEAR):
                    p = block * PB + d * NEAR + k
                    low = [edge_v[f, p, pl.ds(2 * b, ROWS, stride=0), :] for b in range(4)]
                    top = [edge_v[f, p, pl.ds(2 * b + 1, ROWS, stride=0), :] for b in range(4)]
                    low = [low[1], low[2], low[3], low[3], jnp.where(small, low[0], low[2])]
                    top = [top[1], top[2], top[3], top[3], jnp.where(small, top[0], top[2])]
                    x = [part_v[f, p, v] + u_low[v] * low[v] + u_top[v] * top[v] for v in range(PACK)]
                    s, spare = fold(x, m, lane, even, small)
                    at = f * NEAR + k
                    for b in range(4):
                        out_v[dest, at * 4 + b] = s[b]
                    extra = jnp.where(lane == at, spare, extra)
            out_v[dest, SENT - 1] = extra
        out_copy(block).start()
        return carry

    lax.fori_loop(0, BLOCKS, step, 0)
    wait_all(out_copy, BLOCKS)


SENT_V = pltpu.VMEM((GROUPS, SENT, ROWS, LANES), F32)


def pack(slot, messages, part, edges):
    return pl.pallas_call(
        pack_kernel,
        in_specs=[SCALARS, ANY, ANY, ANY],
        out_specs=ANY,
        out_shape=jax.ShapeDtypeStruct((GROUPS, SENT, ROWS, LANES), F32),
        scratch_shapes=[
            pltpu.VMEM((NSUB, FIELDS * MESSAGE, ROWS, LANES), F32),
            pltpu.VMEM((NSUB + 1, FIELDS, PACK, ROWS, LANES), F32),
            PACKED_V,
            EDGE_V,
            SENT_V,
            pltpu.SemaphoreType.DMA,
            dma(BLOCKS),
            pltpu.SemaphoreType.DMA,
            dma(BLOCKS),
        ],
        name="pack",
    )(slot, messages, part, edges)


STEPS = 8
FROM = GROUPS // STEPS


def unpack_kernel(in_hbm, out_hbm, in_v, out_v, in_sem, out_sem):
    def in_copy(i):
        rows = pl.ds(i * FROM, FROM)
        return pltpu.make_async_copy(in_hbm.at[rows], in_v.at[rows], in_sem.at[i])

    def out_copy(i):
        rows = pl.ds(pl.multiple_of(i * FROM * ROWS, ROWS), FROM * ROWS)
        return pltpu.make_async_copy(out_v.at[:, :, :, rows, :], out_hbm.at[:, :, :, rows, :], out_sem.at[i])

    start_all(in_copy, STEPS)
    lane = lane_iota()
    even = row_iota() % 2 == 0

    def step(i, carry):
        in_copy(i).wait()
        for d in range(FROM):
            g = i * FROM + d
            extras = in_v[g, SENT - 1]
            m = column(extras, FIELDS * NEAR).astype(jnp.int32)
            small = m < LANES
            rows = pl.ds(pl.multiple_of(g * ROWS, ROWS), ROWS)
            for f in range(FIELDS):
                for k in range(NEAR):
                    at = f * NEAR + k
                    s = [in_v[g, at * 4 + b] for b in range(4)]
                    tiles = unfold(s, column(extras, at), m, lane, even, small)
                    for c in range(2):
                        for b in range(4):
                            out_v[f, k, c, rows, b * LANES:(b + 1) * LANES] = tiles[c][b]
        out_copy(i).start()
        return carry

    lax.fori_loop(0, STEPS, step, 0)
    wait_all(out_copy, STEPS)


def unpack(received):
    return pl.pallas_call(
        unpack_kernel,
        in_specs=[ANY],
        out_specs=ANY,
        out_shape=jax.ShapeDtypeStruct((FIELDS, NEAR, 2, GROUPS * ROWS, 512), F32),
        scratch_shapes=[
            SENT_V,
            pltpu.VMEM((FIELDS, NEAR, 2, GROUPS * ROWS, 512), F32),
            dma(STEPS),
            dma(STEPS),
        ],
        name="unpack",
    )(received)


def over_ma(sent):
    flat = sent.reshape(GROUPS, SENT * ROWS, LANES)
    received = lax.all_to_all(flat, "ma", split_axis=0, concat_axis=0, tiled=True)
    return received.reshape(GROUPS, SENT, ROWS, LANES)


def body(forcing, slot_wavenumber, inverse, edge_weights):
    inverse = inverse.reshape(FIELDS, POINTS, POINTS // ROWS, ROWS, 512)
    packed, messages = slopes(slot_wavenumber, edge_weights, inverse, forcing)
    messages = lax.all_to_all(messages, "sub", split_axis=0, concat_axis=0, tiled=True)
    part, edges = particular(slot_wavenumber, inverse, packed)
    sent = pack(slot_wavenumber, messages, part, edges)
    return unpack(over_ma(sent))


def solution(mesh):
    return jax.shard_map(
        body,
        mesh=mesh,
        in_specs=(
            P(None, "sub", None, "ma", None),
            P("ma"),
            P("sub", None, None, None, None),
            P("sub", None, None),
        ),
        out_specs=P(None, ("sub", "ma"), None, None, None),
        check_vma=False,
    )
```

```python
import jax
import jax.numpy as jnp
from jax import lax
from jax.experimental import pallas as pl
from jax.experimental.pallas import tpu as pltpu
from jax.sharding import PartitionSpec as P

F32 = jnp.float32
POINTS = 64
FIELDS = 2
NSUB = 8
GROUPS = 16
LANES = 128
ROWS = 8
PACK = 5
QB = 8
PB = 8
NEAR = POINTS // GROUPS
SENT = FIELDS * NEAR * 4 + 1
MESSAGE = 2 * PACK + 2
BLOCKS = POINTS // PB


def lane_iota():
    return lax.broadcasted_iota(jnp.int32, (ROWS, LANES), 1)


def row_iota():
    return lax.broadcasted_iota(jnp.int32, (ROWS, LANES), 0)


def pair_wavenumber(slot_ref):
    pair = row_iota() // 2
    m = jnp.full((ROWS, LANES), slot_ref[0], jnp.int32)
    for j in range(1, 4):
        m = jnp.where(pair == j, slot_ref[2 * j], m)
    return m


def down(x):
    return pltpu.roll(x, 1, 0)


def up(x):
    return pltpu.roll(x, ROWS - 1, 0)


def fold(x, m, lane, even, small):
    shift = jnp.where(small, m, m - LANES)
    turn = (lane - shift + LANES) % LANES
    below = lane < shift
    low3 = jnp.where(even, x[2], down(x[3]))
    high3 = jnp.where(even, up(x[2]), x[3])
    high3_t = jnp.take_along_axis(high3, turn, axis=1)
    mix_t = jnp.take_along_axis(x[4], turn, axis=1)
    zero = jnp.where(small, jnp.where(below, high3_t, x[4]), jnp.where(below, mix_t, high3_t))
    one = jnp.where(jnp.logical_and(below, jnp.logical_not(small)), high3_t, x[0])
    last = jnp.full((ROWS, LANES), LANES - 1, jnp.int32)
    spare = jnp.take_along_axis(jnp.where(small, high3_t, mix_t), last, axis=1)
    return (zero, one, x[1], low3), spare


def column(x, k):
    return jnp.take_along_axis(x, jnp.full((ROWS, LANES), k, jnp.int32), axis=1)


def unfold(s, spare, m, lane, even, small):
    shift = jnp.where(small, m, m - LANES)
    back = (lane + shift) % LANES
    after = lane >= LANES - shift
    exact = lane == LANES - 1 - shift
    g0 = jnp.take_along_axis(s[0], back, axis=1)
    g1 = jnp.take_along_axis(s[1], back, axis=1)
    value = jnp.where(after, g0, jnp.where(exact, spare, 0.0))
    high3 = jnp.where(small, value, jnp.where(after, g1, g0))
    high2 = jnp.where(small, 0.0, value)
    low0 = jnp.where(lane >= m, s[0], 0.0)
    low1 = jnp.where(lane + LANES >= m, s[1], 0.0)
    lows = [low0, low1, s[2], s[3]]
    first = [jnp.where(even, low0, 0.0), jnp.where(even, low1, 0.0)]
    first += [jnp.where(even, s[2], down(high2)), jnp.where(even, s[3], down(high3))]
    second = [jnp.where(even, up(low0), 0.0), jnp.where(even, up(low1), 0.0)]
    second += [jnp.where(even, up(s[2]), high2), jnp.where(even, up(s[3]), high3)]
    return first, second


AHEAD = 8
EARLY = 3
CHUNKS = FIELDS * BLOCKS


def inverse_chunks(inv_hbm, inv_v, sem):
    def copy(i):
        f = i // BLOCKS
        rows = pl.ds(lax.rem(i, BLOCKS) * PB, PB)
        return pltpu.make_async_copy(inv_hbm.at[f, rows], inv_v.at[f, rows], sem.at[i])

    return copy


def next_chunk(copy, i):
    copy(i).wait()

    @pl.when(i + AHEAD < CHUNKS)
    def _():
        copy(i + AHEAD).start()


def start_all(copy, count, first=0):
    def step(i, carry):
        copy(i).start()
        return carry

    lax.fori_loop(first, first + count, step, 0)


def wait_all(copy, count, first=0):
    def step(i, carry):
        copy(i).wait()
        return carry

    lax.fori_loop(first, count, step, 0)


def slope_kernel(
    slot_ref, weight_ref, inv_hbm, src_hbm, packed_hbm, msg_hbm, part_hbm, edge_hbm,
    inv_v, src_v, packed_v, e_v, msg_ref, part_v, edge_v, odd_v, inv_sem, src_sem, out_sem, msg_sem, early_sem
):
    copy = inverse_chunks(inv_hbm, inv_v, inv_sem)
    sources = [pltpu.make_async_copy(src_hbm.at[f], src_v.at[f], src_sem.at[f]) for f in range(FIELDS)]
    results = [pltpu.make_async_copy(packed_v.at[f], packed_hbm.at[f], out_sem.at[f]) for f in range(FIELDS)]
    rows = pl.ds(0, EARLY * PB)
    early = [
        pltpu.make_async_copy(part_v.at[0, rows], part_hbm, early_sem.at[0]),
        pltpu.make_async_copy(edge_v.at[0, rows], edge_hbm, early_sem.at[1]),
    ]
    sources[0].start()
    start_all(copy, AHEAD)
    m = pair_wavenumber(slot_ref)
    lane = lane_iota()
    even = row_iota() % 2 == 0
    small = m < LANES
    zero = jnp.zeros((ROWS, LANES), F32)
    keep1 = lane + LANES >= m
    keep3 = lane + 3 * LANES >= jnp.where(even, m, 511 - m)
    keep_mix = lane >= jnp.where(small, m, 255 - m)
    for f in range(FIELDS):
        sources[f].wait()

        def pack_points(i, carry):
            for k in range(8):
                pack_point(i * 8 + k)
            return carry

        def pack_point(q):
            s = [[src_v[f, q, c, :, b * LANES:(b + 1) * LANES] for b in range(4)] for c in range(2)]
            first = jnp.where(even, s[0][0], down(s[1][0]))
            late = jnp.where(even, up(s[0][2]), s[1][2])
            packed_v[f, q, 0] = jnp.where(keep1, jnp.where(even, s[0][1], down(s[1][1])), 0.0)
            packed_v[f, q, 1] = jnp.where(even, s[0][2], down(s[1][2]))
            packed_v[f, q, 2] = jnp.where(keep3, s[0][3], 0.0)
            packed_v[f, q, 3] = jnp.where(keep3, s[1][3], 0.0)
            packed_v[f, q, 4] = jnp.where(keep_mix, jnp.where(small, first, late), 0.0)

        lax.fori_loop(0, POINTS // 8, pack_points, 0)
        for q in (0, POINTS - 1):
            for v in range(PACK):
                packed_v[f, q, v] = zero
        results[f].start()
        if f + 1 < FIELDS:
            sources[f + 1].start()

        for r in range(2):
            for qb in range(POINTS // ROWS):
                for b in range(4):
                    e_v[r, qb, b] = zero

        def weigh(block, carry):
            next_chunk(copy, f * BLOCKS + block)
            weights = [[weight_ref[0, r, block * PB + p] for p in range(PB)] for r in range(2)]

            def tile_row(qb, carry):
                for b in range(4):
                    low, top = e_v[0, qb, b], e_v[1, qb, b]
                    for p in range(PB):
                        tile = inv_v[f, block * PB + p, qb, :, b * LANES:(b + 1) * LANES]
                        low = low + weights[0][p] * tile
                        top = top + weights[1][p] * tile
                    e_v[0, qb, b] = low
                    e_v[1, qb, b] = top
                return carry

            return lax.fori_loop(0, POINTS // ROWS, tile_row, carry, unroll=2)

        def weigh_and_solve(block, carry):
            weigh(block, carry)
            solve_block(f, inv_v, packed_v, block, small, odd_v, part_v, edge_v)
            return carry

        if f == 0:
            lax.fori_loop(0, EARLY, weigh_and_solve, 0)
            for copy_out in early:
                copy_out.start()
            lax.fori_loop(EARLY, BLOCKS, weigh, 0)
        else:
            lax.fori_loop(0, BLOCKS, weigh, 0)

        def accumulate(qb, sums):
            sums = list(sums)
            for row in range(ROWS):
                x = [packed_v[f, qb * ROWS + row, v] for v in range(PACK)]
                for r in range(2):
                    e = [jnp.broadcast_to(e_v[r, qb, b, row:row + 1, :], (ROWS, LANES)) for b in range(4)]
                    e = [e[1], e[2], e[3], e[3], jnp.where(small, e[0], e[2])]
                    for v in range(PACK):
                        sums[r * PACK + v] = sums[r * PACK + v] + e[v] * x[v]
            return tuple(sums)

        sums = lax.fori_loop(0, POINTS // ROWS, accumulate, (zero,) * (2 * PACK))
        for i in range(2 * PACK):
            msg_ref[f * MESSAGE + i] = sums[i]
        for r in range(2):
            for b in range(4):
                msg_ref[f * MESSAGE + 2 * PACK + r, 2 * b:2 * b + 1, :] = e_v[r, 0, b, 0:1, :]
                msg_ref[f * MESSAGE + 2 * PACK + r, 2 * b + 1:2 * b + 2, :] = (
                    e_v[r, POINTS // ROWS - 1, b, ROWS - 1:ROWS, :]
                )

    def message_copy(k):
        return pltpu.make_async_copy(msg_ref, msg_hbm.at[k], msg_sem.at[k])

    start_all(message_copy, NSUB)
    for copy_out in results + early:
        copy_out.wait()
    wait_all(message_copy, NSUB)


ANY = pl.BlockSpec(memory_space=pl.ANY)
SCALARS = pl.BlockSpec(memory_space=pltpu.SMEM)
INVERSE_V = pltpu.VMEM((FIELDS, POINTS, POINTS // ROWS, ROWS, 512), F32)
PACKED_V = pltpu.VMEM((FIELDS, POINTS, PACK, ROWS, LANES), F32)
EDGE_V = pltpu.VMEM((FIELDS, POINTS, ROWS, LANES), F32)


def dma(*shape):
    return pltpu.SemaphoreType.DMA(shape)


def slopes(slot, weights, inverse, forcing):
    return pl.pallas_call(
        slope_kernel,
        in_specs=[SCALARS, SCALARS, ANY, ANY],
        out_specs=[ANY] * 4,
        out_shape=[
            jax.ShapeDtypeStruct((FIELDS, POINTS, PACK, ROWS, LANES), F32),
            jax.ShapeDtypeStruct((NSUB, FIELDS * MESSAGE, ROWS, LANES), F32),
            jax.ShapeDtypeStruct((EARLY * PB, PACK, ROWS, LANES), F32),
            jax.ShapeDtypeStruct((EARLY * PB, ROWS, LANES), F32),
        ],
        scratch_shapes=[
            INVERSE_V,
            pltpu.VMEM((FIELDS, POINTS, 2, ROWS, 512), F32),
            pltpu.VMEM((FIELDS, POINTS, PACK, ROWS, LANES), F32),
            pltpu.VMEM((2, POINTS // ROWS, 4, ROWS, LANES), F32),
            pltpu.VMEM((FIELDS * MESSAGE, ROWS, LANES), F32),
            pltpu.VMEM((1, EARLY * PB, PACK, ROWS, LANES), F32),
            pltpu.VMEM((1, EARLY * PB, ROWS, LANES), F32),
            pltpu.VMEM((3 * PB, ROWS, LANES), F32),
            dma(CHUNKS),
            dma(FIELDS),
            dma(FIELDS),
            dma(NSUB),
            dma(2),
        ],
        cost_estimate=pl.CostEstimate(flops=20_000_000, bytes_accessed=24_000_000, transcendentals=0),
        name="slopes",
    )(slot, weights, inverse, forcing)


def block_sums(f, inv_v, packed_v, block, small, odd_v):
    zero = jnp.zeros((ROWS, LANES), F32)

    def unit(p, qb, r, b):
        line = inv_v[f, block * PB + p, qb, r:r + 1, b * LANES:(b + 1) * LANES]
        return jnp.broadcast_to(line, (ROWS, LANES))

    def odd_rows(qb, sums, rows):
        sums = list(sums)
        for r in rows:
            s = [packed_v[f, qb * ROWS + r, v] for v in (0, 2, 3)]
            for p in range(PB):
                one = unit(p, qb, r, 1)
                three = unit(p, qb, r, 3)
                sums[3 * p] = sums[3 * p] + one * s[0]
                sums[3 * p + 1] = sums[3 * p + 1] + three * s[1]
                sums[3 * p + 2] = sums[3 * p + 2] + three * s[2]
        return tuple(sums)

    def even_rows(qb, sums, rows):
        sums = list(sums)
        for r in rows:
            s = [packed_v[f, qb * ROWS + r, v] for v in (1, 4)]
            for p in range(PB):
                none = unit(p, qb, r, 0)
                two = unit(p, qb, r, 2)
                sums[2 * p] = sums[2 * p] + two * s[0]
                sums[2 * p + 1] = sums[2 * p + 1] + jnp.where(small, none, two) * s[1]
        return tuple(sums)

    def all_rows(rows_of, sums):
        last = POINTS // ROWS - 1
        sums = rows_of(0, sums, range(1, ROWS))
        sums = lax.fori_loop(1, last, lambda qb, c: rows_of(qb, c, range(ROWS)), sums)
        return rows_of(last, sums, range(ROWS - 1))

    odd = all_rows(odd_rows, (zero,) * (3 * PB))
    for i in range(3 * PB):
        odd_v[i] = odd[i]
    even = all_rows(even_rows, (zero,) * (2 * PB))
    return [[odd_v[3 * p], even[2 * p], odd_v[3 * p + 1], odd_v[3 * p + 2], even[2 * p + 1]] for p in range(PB)]


def solve_block(f, inv_v, packed_v, block, small, odd_v, part_v, edge_v):
    x = block_sums(f, inv_v, packed_v, block, small, odd_v)
    for p in range(PB):
        at = block * PB + p
        for v in range(PACK):
            part_v[f, at, v] = x[p][v]
        for b in range(4):
            lanes = slice(b * LANES, (b + 1) * LANES)
            edge_v[f, at, 2 * b:2 * b + 1, :] = inv_v[f, at, 0, 0:1, lanes]
            edge_v[f, at, 2 * b + 1:2 * b + 2, :] = inv_v[f, at, POINTS // ROWS - 1, ROWS - 1:ROWS, lanes]


def particular_kernel(
    slot_ref, inv_hbm, packed_hbm, part_hbm, edge_hbm, inv_v, packed_v, part_v, edge_v, odd_v, inv_sem, src_sem, part_sem, edge_sem
):
    copy = inverse_chunks(inv_hbm, inv_v, inv_sem)
    sources = [pltpu.make_async_copy(packed_hbm.at[f], packed_v.at[f], src_sem.at[f]) for f in range(FIELDS)]
    sources[0].start()
    start_all(copy, AHEAD, EARLY)
    small = pair_wavenumber(slot_ref) < LANES

    def part_copy(i):
        f, rows = i // BLOCKS, pl.ds(lax.rem(i, BLOCKS) * PB, PB)
        return pltpu.make_async_copy(part_v.at[f, rows], part_hbm.at[f, rows], part_sem.at[i])

    edges = []
    for f in range(FIELDS):
        late = pl.ds(EARLY * PB if f == 0 else 0, POINTS - (EARLY * PB if f == 0 else 0))
        edges.append(pltpu.make_async_copy(edge_v.at[f, late], edge_hbm.at[f, late], edge_sem.at[f]))
    for f in range(FIELDS):
        sources[f].wait()
        if f + 1 < FIELDS:
            sources[f + 1].start()

        def step(block, carry):
            next_chunk(copy, f * BLOCKS + block)
            solve_block(f, inv_v, packed_v, block, small, odd_v, part_v, edge_v)
            part_copy(f * BLOCKS + block).start()
            return carry

        lax.fori_loop(EARLY if f == 0 else 0, BLOCKS, step, 0)
        edges[f].start()
    wait_all(part_copy, CHUNKS, EARLY)
    for edge in edges:
        edge.wait()


def particular(slot, inverse, packed):
    return pl.pallas_call(
        particular_kernel,
        in_specs=[SCALARS, ANY, ANY],
        out_specs=[ANY, ANY],
        out_shape=[
            jax.ShapeDtypeStruct((FIELDS, POINTS, PACK, ROWS, LANES), F32),
            jax.ShapeDtypeStruct((FIELDS, POINTS, ROWS, LANES), F32),
        ],
        scratch_shapes=[
            INVERSE_V,
            PACKED_V,
            PACKED_V,
            EDGE_V,
            pltpu.VMEM((3 * PB, ROWS, LANES), F32),
            dma(CHUNKS),
            dma(FIELDS),
            dma(CHUNKS),
            dma(FIELDS),
        ],
        cost_estimate=pl.CostEstimate(flops=90_000_000, bytes_accessed=24_000_000, transcendentals=0),
        name="particular",
    )(slot, inverse, packed)


def solve_interface(f, all_v, u_v, small):
    base = f * MESSAGE
    zero = jnp.zeros((ROWS, LANES), F32)
    for v in range(PACK):
        u_v[0, f, v] = zero
        u_v[NSUB, f, v] = zero

    def coefficient(t, r, k, b):
        return all_v[t, base + 2 * PACK + r, pl.ds(2 * b + k, ROWS, stride=0), :]

    ratio = [zero] * PACK
    reduced = [zero] * PACK
    ratios = []
    reduceds = []
    for level in range(NSUB - 1):
        factors = []
        for b in range(4):
            lower = coefficient(level, 1, 0, b)
            middle = coefficient(level, 1, 1, b) - coefficient(level + 1, 0, 0, b)
            upper = -coefficient(level + 1, 0, 1, b)
            factors.append((lower, middle, upper))
        mixed = tuple(jnp.where(small, x, y) for x, y in zip(factors[0], factors[2]))
        new_ratio, new_reduced = [None] * PACK, [None] * PACK
        for v, (lower, middle, upper) in enumerate((factors[1], factors[2], factors[3], factors[3], mixed)):
            right = all_v[level + 1, base + v] - all_v[level, base + PACK + v]
            inverted = last if v == 3 else 1.0 / (middle - lower * ratio[v])
            last = inverted
            new_ratio[v] = upper * inverted
            new_reduced[v] = (right - lower * reduced[v]) * inverted
        ratio, reduced = new_ratio, new_reduced
        ratios.append(ratio)
        reduceds.append(reduced)
    later = [zero] * PACK
    for level in range(NSUB - 2, -1, -1):
        later = [reduceds[level][v] - ratios[level][v] * later[v] for v in range(PACK)]
        for v in range(PACK):
            u_v[level + 1, f, v] = later[v]


PER = PB // NEAR


def pack_kernel(
    slot_ref, all_hbm, early_part, early_edge, part_hbm, edge_hbm, out_hbm,
    all_v, u_v, part_v, edge_v, out_v, all_sem, part_sem, edge_sem, early_sem, out_sem
):
    messages = pltpu.make_async_copy(all_hbm, all_v, all_sem)
    messages.start()
    rows = pl.ds(0, EARLY * PB)
    late = pl.ds(EARLY * PB, POINTS - EARLY * PB)
    edges = [
        pltpu.make_async_copy(early_edge, edge_v.at[0, rows], edge_sem.at[0]),
        pltpu.make_async_copy(edge_hbm.at[0, late], edge_v.at[0, late], edge_sem.at[1]),
        pltpu.make_async_copy(edge_hbm.at[1], edge_v.at[1], edge_sem.at[2]),
    ]
    for edge in edges:
        edge.start()

    def first_copy(i):
        rows = pl.ds(i * PB, PB)
        return pltpu.make_async_copy(early_part.at[rows], part_v.at[0, rows], early_sem.at[i])

    def late_copy(i):
        rows = pl.ds(i * PB, PB)
        return pltpu.make_async_copy(part_hbm.at[0, rows], part_v.at[0, rows], early_sem.at[i])

    def part_copy(i):
        rows = pl.ds(i * PB, PB)
        return pltpu.make_async_copy(part_hbm.at[1, rows], part_v.at[1, rows], part_sem.at[i])

    start_all(first_copy, EARLY)
    start_all(part_copy, EARLY)
    start_all(late_copy, BLOCKS - EARLY, EARLY)
    start_all(part_copy, BLOCKS - EARLY, EARLY)
    m = pair_wavenumber(slot_ref)
    lane = lane_iota()
    even = row_iota() % 2 == 0
    small = m < LANES
    messages.wait()
    for f in range(FIELDS):
        solve_interface(f, all_v, u_v, small)
    for edge in edges:
        edge.wait()
    sub = lax.axis_index("sub")

    def out_copy(i):
        rows = pl.ds(i * PER, PER)
        return pltpu.make_async_copy(out_v.at[rows], out_hbm.at[rows], out_sem.at[i])

    def step(block, carry):
        late_copy(block).wait()
        part_copy(block).wait()
        for d in range(PER):
            dest = block * PER + d
            extra = jnp.where(lane == FIELDS * NEAR, m.astype(F32), 0.0)
            for f in range(FIELDS):
                u_low = [u_v[sub, f, v] for v in range(PACK)]
                u_top = [u_v[sub + 1, f, v] for v in range(PACK)]
                for k in range(NEAR):
                    p = block * PB + d * NEAR + k
                    low = [edge_v[f, p, pl.ds(2 * b, ROWS, stride=0), :] for b in range(4)]
                    top = [edge_v[f, p, pl.ds(2 * b + 1, ROWS, stride=0), :] for b in range(4)]
                    low = [low[1], low[2], low[3], low[3], jnp.where(small, low[0], low[2])]
                    top = [top[1], top[2], top[3], top[3], jnp.where(small, top[0], top[2])]
                    x = [part_v[f, p, v] + u_low[v] * low[v] + u_top[v] * top[v] for v in range(PACK)]
                    s, spare = fold(x, m, lane, even, small)
                    at = f * NEAR + k
                    for b in range(4):
                        out_v[dest, at * 4 + b] = s[b]
                    extra = jnp.where(lane == at, spare, extra)
            out_v[dest, SENT - 1] = extra
        out_copy(block).start()
        return carry

    lax.fori_loop(0, BLOCKS, step, 0)
    wait_all(out_copy, BLOCKS)


SENT_V = pltpu.VMEM((GROUPS, SENT, ROWS, LANES), F32)


def pack(slot, messages, early_part, early_edge, part, edges):
    return pl.pallas_call(
        pack_kernel,
        in_specs=[SCALARS] + [ANY] * 5,
        out_specs=ANY,
        out_shape=jax.ShapeDtypeStruct((GROUPS, SENT, ROWS, LANES), F32),
        scratch_shapes=[
            pltpu.VMEM((NSUB, FIELDS * MESSAGE, ROWS, LANES), F32),
            pltpu.VMEM((NSUB + 1, FIELDS, PACK, ROWS, LANES), F32),
            PACKED_V,
            EDGE_V,
            SENT_V,
            pltpu.SemaphoreType.DMA,
            dma(BLOCKS),
            dma(3),
            dma(BLOCKS),
            dma(BLOCKS),
        ],
        name="pack",
    )(slot, messages, early_part, early_edge, part, edges)


STEPS = 8
FROM = GROUPS // STEPS


def unpack_kernel(in_hbm, out_hbm, in_v, out_v, in_sem, out_sem):
    def in_copy(i):
        rows = pl.ds(i * FROM, FROM)
        return pltpu.make_async_copy(in_hbm.at[rows], in_v.at[rows], in_sem.at[i])

    def out_copy(i):
        rows = pl.ds(pl.multiple_of(i * FROM * ROWS, ROWS), FROM * ROWS)
        return pltpu.make_async_copy(out_v.at[:, :, :, rows, :], out_hbm.at[:, :, :, rows, :], out_sem.at[i])

    start_all(in_copy, STEPS)
    lane = lane_iota()
    even = row_iota() % 2 == 0

    def step(i, carry):
        in_copy(i).wait()
        for d in range(FROM):
            g = i * FROM + d
            extras = in_v[g, SENT - 1]
            m = column(extras, FIELDS * NEAR).astype(jnp.int32)
            small = m < LANES
            rows = pl.ds(pl.multiple_of(g * ROWS, ROWS), ROWS)
            for f in range(FIELDS):
                for k in range(NEAR):
                    at = f * NEAR + k
                    s = [in_v[g, at * 4 + b] for b in range(4)]
                    tiles = unfold(s, column(extras, at), m, lane, even, small)
                    for c in range(2):
                        for b in range(4):
                            out_v[f, k, c, rows, b * LANES:(b + 1) * LANES] = tiles[c][b]
        out_copy(i).start()
        return carry

    lax.fori_loop(0, STEPS, step, 0)
    wait_all(out_copy, STEPS)


def unpack(received):
    return pl.pallas_call(
        unpack_kernel,
        in_specs=[ANY],
        out_specs=ANY,
        out_shape=jax.ShapeDtypeStruct((FIELDS, NEAR, 2, GROUPS * ROWS, 512), F32),
        scratch_shapes=[
            SENT_V,
            pltpu.VMEM((FIELDS, NEAR, 2, GROUPS * ROWS, 512), F32),
            dma(STEPS),
            dma(STEPS),
        ],
        name="unpack",
    )(received)


def over_ma(sent):
    flat = sent.reshape(GROUPS, SENT * ROWS, LANES)
    received = lax.all_to_all(flat, "ma", split_axis=0, concat_axis=0, tiled=True)
    return received.reshape(GROUPS, SENT, ROWS, LANES)


def body(forcing, slot_wavenumber, inverse, edge_weights):
    inverse = inverse.reshape(FIELDS, POINTS, POINTS // ROWS, ROWS, 512)
    packed, messages, early_part, early_edge = slopes(slot_wavenumber, edge_weights, inverse, forcing)
    messages = lax.all_to_all(messages, "sub", split_axis=0, concat_axis=0, tiled=True)
    part, edges = particular(slot_wavenumber, inverse, packed)
    sent = pack(slot_wavenumber, messages, early_part, early_edge, part, edges)
    return unpack(over_ma(sent))


def solution(mesh):
    return jax.shard_map(
        body,
        mesh=mesh,
        in_specs=(
            P(None, "sub", None, "ma", None),
            P("ma"),
            P("sub", None, None, None, None),
            P("sub", None, None),
        ),
        out_specs=P(None, ("sub", "ma"), None, None, None),
        check_vma=False,
    )
```

```python
import jax
import jax.numpy as jnp
from jax import lax
from jax.experimental import pallas as pl
from jax.experimental.pallas import tpu as pltpu
from jax.sharding import PartitionSpec as P

F32 = jnp.float32
POINTS = 64
FIELDS = 2
NSUB = 8
GROUPS = 16
LANES = 128
ROWS = 8
PACK = 5
QB = 8
PB = 8
NEAR = POINTS // GROUPS
SENT = FIELDS * NEAR * 4 + 1
MESSAGE = 2 * PACK + 2
BLOCKS = POINTS // PB


def lane_iota():
    return lax.broadcasted_iota(jnp.int32, (ROWS, LANES), 1)


def row_iota():
    return lax.broadcasted_iota(jnp.int32, (ROWS, LANES), 0)


def pair_wavenumber(slot_ref):
    pair = row_iota() // 2
    m = jnp.full((ROWS, LANES), slot_ref[0], jnp.int32)
    for j in range(1, 4):
        m = jnp.where(pair == j, slot_ref[2 * j], m)
    return m


def down(x):
    return pltpu.roll(x, 1, 0)


def up(x):
    return pltpu.roll(x, ROWS - 1, 0)


def fold(x, m, lane, even, small):
    shift = jnp.where(small, m, m - LANES)
    turn = (lane - shift + LANES) % LANES
    below = lane < shift
    low3 = jnp.where(even, x[2], down(x[3]))
    high3 = jnp.where(even, up(x[2]), x[3])
    high3_t = jnp.take_along_axis(high3, turn, axis=1)
    mix_t = jnp.take_along_axis(x[4], turn, axis=1)
    zero = jnp.where(small, jnp.where(below, high3_t, x[4]), jnp.where(below, mix_t, high3_t))
    one = jnp.where(jnp.logical_and(below, jnp.logical_not(small)), high3_t, x[0])
    last = jnp.full((ROWS, LANES), LANES - 1, jnp.int32)
    spare = jnp.take_along_axis(jnp.where(small, high3_t, mix_t), last, axis=1)
    return (zero, one, x[1], low3), spare


def column(x, k):
    return jnp.take_along_axis(x, jnp.full((ROWS, LANES), k, jnp.int32), axis=1)


def unfold(s, spare, m, lane, even, small):
    shift = jnp.where(small, m, m - LANES)
    back = (lane + shift) % LANES
    after = lane >= LANES - shift
    exact = lane == LANES - 1 - shift
    g0 = jnp.take_along_axis(s[0], back, axis=1)
    g1 = jnp.take_along_axis(s[1], back, axis=1)
    value = jnp.where(after, g0, jnp.where(exact, spare, 0.0))
    high3 = jnp.where(small, value, jnp.where(after, g1, g0))
    high2 = jnp.where(small, 0.0, value)
    low0 = jnp.where(lane >= m, s[0], 0.0)
    low1 = jnp.where(lane + LANES >= m, s[1], 0.0)
    lows = [low0, low1, s[2], s[3]]
    first = [jnp.where(even, low0, 0.0), jnp.where(even, low1, 0.0)]
    first += [jnp.where(even, s[2], down(high2)), jnp.where(even, s[3], down(high3))]
    second = [jnp.where(even, up(low0), 0.0), jnp.where(even, up(low1), 0.0)]
    second += [jnp.where(even, up(s[2]), high2), jnp.where(even, up(s[3]), high3)]
    return first, second


AHEAD = 8
EARLY = 3
PARTICULAR_MIB = 24
PACK_MIB = 4
UNPACK_MIB = 8
KEPT = PACK + 1
CHUNKS = FIELDS * BLOCKS


def inverse_chunks(inv_hbm, inv_v, sem):
    def copy(i):
        f = i // BLOCKS
        rows = pl.ds(lax.rem(i, BLOCKS) * PB, PB)
        return pltpu.make_async_copy(inv_hbm.at[f, rows], inv_v.at[f, rows], sem.at[i])

    return copy


def next_chunk(copy, i):
    copy(i).wait()

    @pl.when(i + AHEAD < CHUNKS)
    def _():
        copy(i + AHEAD).start()


def start_all(copy, count, first=0):
    def step(i, carry):
        copy(i).start()
        return carry

    lax.fori_loop(first, first + count, step, 0)


def wait_all(copy, count, first=0):
    def step(i, carry):
        copy(i).wait()
        return carry

    lax.fori_loop(first, count, step, 0)


def slope_kernel(
    slot_ref, weight_ref, inv_hbm, src_hbm, packed_hbm, msg_hbm, part_hbm,
    inv_v, src_v, packed_v, e_v, msg_ref, part_v, odd_v, inv_sem, src_sem, out_sem, msg_sem, early_sem
):
    copy = inverse_chunks(inv_hbm, inv_v, inv_sem)
    sources = [pltpu.make_async_copy(src_hbm.at[f], src_v.at[f], src_sem.at[f]) for f in range(FIELDS)]
    results = [pltpu.make_async_copy(packed_v.at[f], packed_hbm.at[f], out_sem.at[f]) for f in range(FIELDS)]
    rows = pl.ds(0, EARLY * PB)
    early = [pltpu.make_async_copy(part_v.at[0, rows], part_hbm, early_sem)]
    sources[0].start()
    start_all(copy, AHEAD)
    m = pair_wavenumber(slot_ref)
    lane = lane_iota()
    even = row_iota() % 2 == 0
    small = m < LANES
    zero = jnp.zeros((ROWS, LANES), F32)
    keep1 = lane + LANES >= m
    keep3 = lane + 3 * LANES >= jnp.where(even, m, 511 - m)
    keep_mix = lane >= jnp.where(small, m, 255 - m)
    for f in range(FIELDS):
        sources[f].wait()

        def pack_points(i, carry):
            for k in range(8):
                pack_point(i * 8 + k)
            return carry

        def pack_point(q):
            s = [[src_v[f, q, c, :, b * LANES:(b + 1) * LANES] for b in range(4)] for c in range(2)]
            first = jnp.where(even, s[0][0], down(s[1][0]))
            late = jnp.where(even, up(s[0][2]), s[1][2])
            packed_v[f, q, 0] = jnp.where(keep1, jnp.where(even, s[0][1], down(s[1][1])), 0.0)
            packed_v[f, q, 1] = jnp.where(even, s[0][2], down(s[1][2]))
            packed_v[f, q, 2] = jnp.where(keep3, s[0][3], 0.0)
            packed_v[f, q, 3] = jnp.where(keep3, s[1][3], 0.0)
            packed_v[f, q, 4] = jnp.where(keep_mix, jnp.where(small, first, late), 0.0)

        lax.fori_loop(0, POINTS // 8, pack_points, 0)
        for q in (0, POINTS - 1):
            for v in range(PACK):
                packed_v[f, q, v] = zero
        results[f].start()
        if f + 1 < FIELDS:
            sources[f + 1].start()

        for r in range(2):
            for qb in range(POINTS // ROWS):
                for b in range(4):
                    e_v[r, qb, b] = zero

        def weigh(block, carry):
            next_chunk(copy, f * BLOCKS + block)
            weights = [[weight_ref[0, r, block * PB + p] for p in range(PB)] for r in range(2)]

            def tile_row(qb, carry):
                for b in range(4):
                    low, top = e_v[0, qb, b], e_v[1, qb, b]
                    for p in range(PB):
                        tile = inv_v[f, block * PB + p, qb, :, b * LANES:(b + 1) * LANES]
                        low = low + weights[0][p] * tile
                        top = top + weights[1][p] * tile
                    e_v[0, qb, b] = low
                    e_v[1, qb, b] = top
                return carry

            return lax.fori_loop(0, POINTS // ROWS, tile_row, carry, unroll=2)

        def weigh_and_solve(block, carry):
            weigh(block, carry)
            solve_block(f, inv_v, packed_v, block, small, odd_v, part_v)
            return carry

        if f == 0:
            lax.fori_loop(0, EARLY, weigh_and_solve, 0)
            for copy_out in early:
                copy_out.start()
            lax.fori_loop(EARLY, BLOCKS, weigh, 0)
        else:
            lax.fori_loop(0, BLOCKS, weigh, 0)

        def accumulate(qb, sums):
            sums = list(sums)
            for row in range(ROWS):
                x = [packed_v[f, qb * ROWS + row, v] for v in range(PACK)]
                for r in range(2):
                    e = [jnp.broadcast_to(e_v[r, qb, b, row:row + 1, :], (ROWS, LANES)) for b in range(4)]
                    e = [e[1], e[2], e[3], e[3], jnp.where(small, e[0], e[2])]
                    for v in range(PACK):
                        sums[r * PACK + v] = sums[r * PACK + v] + e[v] * x[v]
            return tuple(sums)

        sums = lax.fori_loop(0, POINTS // ROWS, accumulate, (zero,) * (2 * PACK))
        for i in range(2 * PACK):
            msg_ref[f * MESSAGE + i] = sums[i]
        for r in range(2):
            for b in range(4):
                msg_ref[f * MESSAGE + 2 * PACK + r, 2 * b:2 * b + 1, :] = e_v[r, 0, b, 0:1, :]
                msg_ref[f * MESSAGE + 2 * PACK + r, 2 * b + 1:2 * b + 2, :] = (
                    e_v[r, POINTS // ROWS - 1, b, ROWS - 1:ROWS, :]
                )

    def message_copy(k):
        return pltpu.make_async_copy(msg_ref, msg_hbm.at[k], msg_sem.at[k])

    start_all(message_copy, NSUB)
    for copy_out in results + early:
        copy_out.wait()
    wait_all(message_copy, NSUB)


ANY = pl.BlockSpec(memory_space=pl.ANY)
SCALARS = pl.BlockSpec(memory_space=pltpu.SMEM)
INVERSE_V = pltpu.VMEM((FIELDS, POINTS, POINTS // ROWS, ROWS, 512), F32)
PACKED_V = pltpu.VMEM((FIELDS, POINTS, PACK, ROWS, LANES), F32)
PART_V = pltpu.VMEM((FIELDS, POINTS, KEPT, ROWS, LANES), F32)
SENT_V = pltpu.VMEM((GROUPS, SENT, ROWS, LANES), F32)
IN_VMEM = pl.BlockSpec(memory_space=pltpu.VMEM)
IN_HBM = pl.BlockSpec(memory_space=pltpu.HBM)


def grant(mib):
    return pltpu.CompilerParams(vmem_limit_bytes=mib * 2**20)


def held(x):
    return pltpu.with_memory_space_constraint(x, pltpu.VMEM)


def far(x):
    return pltpu.with_memory_space_constraint(x, pltpu.HBM)


def dma(*shape):
    return pltpu.SemaphoreType.DMA(shape)


def slopes(slot, weights, inverse, forcing):
    return pl.pallas_call(
        slope_kernel,
        in_specs=[SCALARS, SCALARS, ANY, ANY],
        out_specs=[ANY] * 3,
        out_shape=[
            jax.ShapeDtypeStruct((FIELDS, POINTS, PACK, ROWS, LANES), F32),
            jax.ShapeDtypeStruct((NSUB, FIELDS * MESSAGE, ROWS, LANES), F32),
            jax.ShapeDtypeStruct((EARLY * PB, KEPT, ROWS, LANES), F32),
        ],
        scratch_shapes=[
            INVERSE_V,
            pltpu.VMEM((FIELDS, POINTS, 2, ROWS, 512), F32),
            pltpu.VMEM((FIELDS, POINTS, PACK, ROWS, LANES), F32),
            pltpu.VMEM((2, POINTS // ROWS, 4, ROWS, LANES), F32),
            pltpu.VMEM((FIELDS * MESSAGE, ROWS, LANES), F32),
            pltpu.VMEM((1, EARLY * PB, KEPT, ROWS, LANES), F32),
            pltpu.VMEM((3 * PB, ROWS, LANES), F32),
            dma(CHUNKS),
            dma(FIELDS),
            dma(FIELDS),
            dma(NSUB),
            pltpu.SemaphoreType.DMA,
        ],
        cost_estimate=pl.CostEstimate(flops=20_000_000, bytes_accessed=24_000_000, transcendentals=0),
        name="slopes",
    )(slot, weights, inverse, forcing)


def block_sums(f, inv_v, packed_v, block, small, odd_v):
    zero = jnp.zeros((ROWS, LANES), F32)

    def unit(p, qb, r, b):
        line = inv_v[f, block * PB + p, qb, r:r + 1, b * LANES:(b + 1) * LANES]
        return jnp.broadcast_to(line, (ROWS, LANES))

    def odd_rows(qb, sums, rows):
        sums = list(sums)
        for r in rows:
            s = [packed_v[f, qb * ROWS + r, v] for v in (0, 2, 3)]
            for p in range(PB):
                one = unit(p, qb, r, 1)
                three = unit(p, qb, r, 3)
                sums[3 * p] = sums[3 * p] + one * s[0]
                sums[3 * p + 1] = sums[3 * p + 1] + three * s[1]
                sums[3 * p + 2] = sums[3 * p + 2] + three * s[2]
        return tuple(sums)

    def even_rows(qb, sums, rows):
        sums = list(sums)
        for r in rows:
            s = [packed_v[f, qb * ROWS + r, v] for v in (1, 4)]
            for p in range(PB):
                none = unit(p, qb, r, 0)
                two = unit(p, qb, r, 2)
                sums[2 * p] = sums[2 * p] + two * s[0]
                sums[2 * p + 1] = sums[2 * p + 1] + jnp.where(small, none, two) * s[1]
        return tuple(sums)

    def all_rows(rows_of, sums):
        last = POINTS // ROWS - 1
        sums = rows_of(0, sums, range(1, ROWS))
        sums = lax.fori_loop(1, last, lambda qb, c: rows_of(qb, c, range(ROWS)), sums)
        return rows_of(last, sums, range(ROWS - 1))

    odd = all_rows(odd_rows, (zero,) * (3 * PB))
    for i in range(3 * PB):
        odd_v[i] = odd[i]
    even = all_rows(even_rows, (zero,) * (2 * PB))
    return [[odd_v[3 * p], even[2 * p], odd_v[3 * p + 1], odd_v[3 * p + 2], even[2 * p + 1]] for p in range(PB)]


def solve_block(f, inv_v, packed_v, block, small, odd_v, part_v):
    x = block_sums(f, inv_v, packed_v, block, small, odd_v)
    for p in range(PB):
        at = block * PB + p
        for v in range(PACK):
            part_v[f, at, v] = x[p][v]
        for b in range(4):
            lanes = slice(b * LANES, (b + 1) * LANES)
            part_v[f, at, PACK, 2 * b:2 * b + 1, :] = inv_v[f, at, 0, 0:1, lanes]
            part_v[f, at, PACK, 2 * b + 1:2 * b + 2, :] = inv_v[f, at, POINTS // ROWS - 1, ROWS - 1:ROWS, lanes]


def particular_kernel(
    slot_ref, inv_hbm, packed_hbm, early_hbm, part_v, inv_v, packed_v, odd_v, inv_sem, src_sem, early_sem
):
    copy = inverse_chunks(inv_hbm, inv_v, inv_sem)
    sources = [pltpu.make_async_copy(packed_hbm.at[f], packed_v.at[f], src_sem.at[f]) for f in range(FIELDS)]
    early = pltpu.make_async_copy(early_hbm, part_v.at[0, pl.ds(0, EARLY * PB)], early_sem)
    sources[0].start()
    start_all(copy, AHEAD, EARLY)
    early.start()
    small = pair_wavenumber(slot_ref) < LANES
    for f in range(FIELDS):
        sources[f].wait()
        if f + 1 < FIELDS:
            sources[f + 1].start()

        def step(block, carry):
            next_chunk(copy, f * BLOCKS + block)
            solve_block(f, inv_v, packed_v, block, small, odd_v, part_v)
            return carry

        lax.fori_loop(EARLY if f == 0 else 0, BLOCKS, step, 0)
    early.wait()


def particular(slot, inverse, packed, early):
    return pl.pallas_call(
        particular_kernel,
        in_specs=[SCALARS] + [IN_HBM] * 3,
        out_specs=IN_VMEM,
        out_shape=PART_V,
        scratch_shapes=[
            INVERSE_V,
            PACKED_V,
            pltpu.VMEM((3 * PB, ROWS, LANES), F32),
            dma(CHUNKS),
            dma(FIELDS),
            pltpu.SemaphoreType.DMA,
        ],
        compiler_params=grant(PARTICULAR_MIB),
        cost_estimate=pl.CostEstimate(flops=90_000_000, bytes_accessed=24_000_000, transcendentals=0),
        name="particular",
    )(slot, far(inverse), far(packed), far(early))


def solve_interface(f, all_v, u_v, small):
    base = f * MESSAGE
    zero = jnp.zeros((ROWS, LANES), F32)
    for v in range(PACK):
        u_v[0, f, v] = zero
        u_v[NSUB, f, v] = zero

    def coefficient(t, r, k, b):
        return all_v[t, base + 2 * PACK + r, pl.ds(2 * b + k, ROWS, stride=0), :]

    ratio = [zero] * PACK
    reduced = [zero] * PACK
    ratios = []
    reduceds = []
    for level in range(NSUB - 1):
        factors = []
        for b in range(4):
            lower = coefficient(level, 1, 0, b)
            middle = coefficient(level, 1, 1, b) - coefficient(level + 1, 0, 0, b)
            upper = -coefficient(level + 1, 0, 1, b)
            factors.append((lower, middle, upper))
        mixed = tuple(jnp.where(small, x, y) for x, y in zip(factors[0], factors[2]))
        new_ratio, new_reduced = [None] * PACK, [None] * PACK
        for v, (lower, middle, upper) in enumerate((factors[1], factors[2], factors[3], factors[3], mixed)):
            right = all_v[level + 1, base + v] - all_v[level, base + PACK + v]
            inverted = last if v == 3 else 1.0 / (middle - lower * ratio[v])
            last = inverted
            new_ratio[v] = upper * inverted
            new_reduced[v] = (right - lower * reduced[v]) * inverted
        ratio, reduced = new_ratio, new_reduced
        ratios.append(ratio)
        reduceds.append(reduced)
    later = [zero] * PACK
    for level in range(NSUB - 2, -1, -1):
        later = [reduceds[level][v] - ratios[level][v] * later[v] for v in range(PACK)]
        for v in range(PACK):
            u_v[level + 1, f, v] = later[v]


PER = PB // NEAR


def pack_kernel(slot_ref, all_v, part_v, out_v, u_v):
    m = pair_wavenumber(slot_ref)
    lane = lane_iota()
    even = row_iota() % 2 == 0
    small = m < LANES
    for f in range(FIELDS):
        solve_interface(f, all_v, u_v, small)
    sub = lax.axis_index("sub")

    def step(block, carry):
        for d in range(PER):
            dest = block * PER + d
            extra = jnp.where(lane == FIELDS * NEAR, m.astype(F32), 0.0)
            for f in range(FIELDS):
                u_low = [u_v[sub, f, v] for v in range(PACK)]
                u_top = [u_v[sub + 1, f, v] for v in range(PACK)]
                for k in range(NEAR):
                    p = block * PB + d * NEAR + k
                    low = [part_v[f, p, PACK, pl.ds(2 * b, ROWS, stride=0), :] for b in range(4)]
                    top = [part_v[f, p, PACK, pl.ds(2 * b + 1, ROWS, stride=0), :] for b in range(4)]
                    low = [low[1], low[2], low[3], low[3], jnp.where(small, low[0], low[2])]
                    top = [top[1], top[2], top[3], top[3], jnp.where(small, top[0], top[2])]
                    x = [part_v[f, p, v] + u_low[v] * low[v] + u_top[v] * top[v] for v in range(PACK)]
                    s, spare = fold(x, m, lane, even, small)
                    at = f * NEAR + k
                    for b in range(4):
                        out_v[dest, at * 4 + b] = s[b]
                    extra = jnp.where(lane == at, spare, extra)
            out_v[dest, SENT - 1] = extra
        return carry

    lax.fori_loop(0, BLOCKS, step, 0)


def pack(slot, messages, part):
    return pl.pallas_call(
        pack_kernel,
        in_specs=[SCALARS] + [IN_VMEM] * 2,
        out_specs=IN_VMEM,
        out_shape=SENT_V,
        scratch_shapes=[pltpu.VMEM((NSUB + 1, FIELDS, PACK, ROWS, LANES), F32)],
        compiler_params=grant(PACK_MIB),
        name="pack",
    )(slot, held(messages), held(part))


STEPS = 8
FROM = GROUPS // STEPS


def unpack_kernel(in_v, out_hbm, out_v, out_sem):
    def out_copy(i):
        rows = pl.ds(pl.multiple_of(i * FROM * ROWS, ROWS), FROM * ROWS)
        return pltpu.make_async_copy(out_v.at[:, :, :, rows, :], out_hbm.at[:, :, :, rows, :], out_sem.at[i])

    lane = lane_iota()
    even = row_iota() % 2 == 0

    def step(i, carry):
        for d in range(FROM):
            g = i * FROM + d
            extras = in_v[g, SENT - 1]
            m = column(extras, FIELDS * NEAR).astype(jnp.int32)
            small = m < LANES
            rows = pl.ds(pl.multiple_of(g * ROWS, ROWS), ROWS)
            for f in range(FIELDS):
                for k in range(NEAR):
                    at = f * NEAR + k
                    s = [in_v[g, at * 4 + b] for b in range(4)]
                    tiles = unfold(s, column(extras, at), m, lane, even, small)
                    for c in range(2):
                        for b in range(4):
                            out_v[f, k, c, rows, b * LANES:(b + 1) * LANES] = tiles[c][b]
        out_copy(i).start()
        return carry

    lax.fori_loop(0, STEPS, step, 0)
    wait_all(out_copy, STEPS)


def unpack(received):
    return pl.pallas_call(
        unpack_kernel,
        in_specs=[IN_VMEM],
        out_specs=ANY,
        out_shape=jax.ShapeDtypeStruct((FIELDS, NEAR, 2, GROUPS * ROWS, 512), F32),
        scratch_shapes=[pltpu.VMEM((FIELDS, NEAR, 2, GROUPS * ROWS, 512), F32), dma(STEPS)],
        compiler_params=grant(UNPACK_MIB),
        name="unpack",
    )(held(received))


def over_ma(sent):
    flat = sent.reshape(GROUPS, SENT * ROWS, LANES)
    received = lax.all_to_all(flat, "ma", split_axis=0, concat_axis=0, tiled=True)
    return received.reshape(GROUPS, SENT, ROWS, LANES)


def body(forcing, slot_wavenumber, inverse, edge_weights):
    inverse = inverse.reshape(FIELDS, POINTS, POINTS // ROWS, ROWS, 512)
    packed, messages, early = slopes(slot_wavenumber, edge_weights, inverse, forcing)
    messages = lax.all_to_all(messages, "sub", split_axis=0, concat_axis=0, tiled=True)
    part = particular(slot_wavenumber, inverse, packed, early)
    sent = pack(slot_wavenumber, messages, part)
    return unpack(over_ma(sent))


def solution(mesh):
    return jax.shard_map(
        body,
        mesh=mesh,
        in_specs=(
            P(None, "sub", None, "ma", None),
            P("ma"),
            P("sub", None, None, None, None),
            P("sub", None, None),
        ),
        out_specs=P(None, ("sub", "ma"), None, None, None),
        check_vma=False,
    )
```

```python
import jax
import jax.numpy as jnp
from jax import lax
from jax.experimental import pallas as pl
from jax.experimental.pallas import tpu as pltpu
from jax.sharding import PartitionSpec as P

F32 = jnp.float32
POINTS = 64
FIELDS = 2
NSUB = 8
GROUPS = 16
LANES = 128
ROWS = 8
PACK = 5
QB = 8
PB = 8
NEAR = POINTS // GROUPS
SENT = FIELDS * NEAR * 4 + 1
MESSAGE = 2 * PACK + 2
BLOCKS = POINTS // PB


def lane_iota():
    return lax.broadcasted_iota(jnp.int32, (ROWS, LANES), 1)


def row_iota():
    return lax.broadcasted_iota(jnp.int32, (ROWS, LANES), 0)


def pair_wavenumber(slot_ref):
    pair = row_iota() // 2
    m = jnp.full((ROWS, LANES), slot_ref[0], jnp.int32)
    for j in range(1, 4):
        m = jnp.where(pair == j, slot_ref[2 * j], m)
    return m


def down(x):
    return pltpu.roll(x, 1, 0)


def up(x):
    return pltpu.roll(x, ROWS - 1, 0)


def fold(x, m, lane, even, small):
    shift = jnp.where(small, m, m - LANES)
    turn = (lane - shift + LANES) % LANES
    below = lane < shift
    low3 = jnp.where(even, x[2], down(x[3]))
    high3 = jnp.where(even, up(x[2]), x[3])
    high3_t = jnp.take_along_axis(high3, turn, axis=1)
    mix_t = jnp.take_along_axis(x[4], turn, axis=1)
    zero = jnp.where(small, jnp.where(below, high3_t, x[4]), jnp.where(below, mix_t, high3_t))
    one = jnp.where(jnp.logical_and(below, jnp.logical_not(small)), high3_t, x[0])
    last = jnp.full((ROWS, LANES), LANES - 1, jnp.int32)
    spare = jnp.take_along_axis(jnp.where(small, high3_t, mix_t), last, axis=1)
    return (zero, one, x[1], low3), spare


def column(x, k):
    return jnp.take_along_axis(x, jnp.full((ROWS, LANES), k, jnp.int32), axis=1)


def unfold(s, spare, m, lane, even, small):
    shift = jnp.where(small, m, m - LANES)
    back = (lane + shift) % LANES
    after = lane >= LANES - shift
    exact = lane == LANES - 1 - shift
    g0 = jnp.take_along_axis(s[0], back, axis=1)
    g1 = jnp.take_along_axis(s[1], back, axis=1)
    value = jnp.where(after, g0, jnp.where(exact, spare, 0.0))
    high3 = jnp.where(small, value, jnp.where(after, g1, g0))
    high2 = jnp.where(small, 0.0, value)
    low0 = jnp.where(lane >= m, s[0], 0.0)
    low1 = jnp.where(lane + LANES >= m, s[1], 0.0)
    lows = [low0, low1, s[2], s[3]]
    first = [jnp.where(even, low0, 0.0), jnp.where(even, low1, 0.0)]
    first += [jnp.where(even, s[2], down(high2)), jnp.where(even, s[3], down(high3))]
    second = [jnp.where(even, up(low0), 0.0), jnp.where(even, up(low1), 0.0)]
    second += [jnp.where(even, up(s[2]), high2), jnp.where(even, up(s[3]), high3)]
    return first, second


AHEAD = 3
SLOPES_MIB = 18
PARTICULAR_MIB = 4
PACK_MIB = 4
UNPACK_MIB = 8
KEPT = PACK + 1
CHUNKS = FIELDS * BLOCKS


def inverse_chunks(inv_hbm, held_v, sem):
    def copy(i):
        f, block = i // BLOCKS, i % BLOCKS
        rows = pl.ds(block * PB, PB)
        return pltpu.make_async_copy(inv_hbm.at[f, rows], held_v[f].at[rows], sem.at[i])

    return copy


def start_all(copy, count, first=0):
    def step(i, carry):
        copy(i).start()
        return carry

    lax.fori_loop(first, first + count, step, 0)


def wait_all(copy, count, first=0):
    def step(i, carry):
        copy(i).wait()
        return carry

    lax.fori_loop(first, count, step, 0)


def slope_kernel(
    slot_ref, weight_ref, inv_hbm, src_hbm, later_v, packed_v, msg_ref, part_v,
    inv_v, src_v, first_v, e_v, odd_v, inv_sem, src_sem
):
    copy = inverse_chunks(inv_hbm, (inv_v, later_v), inv_sem)
    sources = [pltpu.make_async_copy(src_hbm.at[f], src_v.at[f], src_sem.at[f]) for f in range(FIELDS)]

    sources[0].start()
    copy(0).start()
    m = pair_wavenumber(slot_ref)
    lane = lane_iota()
    even = row_iota() % 2 == 0
    small = m < LANES
    zero = jnp.zeros((ROWS, LANES), F32)
    keep1 = lane + LANES >= m
    keep3 = lane + 3 * LANES >= jnp.where(even, m, 511 - m)
    keep_mix = lane >= jnp.where(small, m, 255 - m)
    for f in range(FIELDS):
        sources[f].wait()
        if f == 0:
            for i in range(1, AHEAD):
                copy(i).start()

        target = first_v if f == 0 else packed_v

        def pack_points(i, carry):
            for k in range(8):
                pack_point(i * 8 + k)
            return carry

        def pack_point(q):
            s = [[src_v[f, q, c, :, b * LANES:(b + 1) * LANES] for b in range(4)] for c in range(2)]
            first = jnp.where(even, s[0][0], down(s[1][0]))
            late = jnp.where(even, up(s[0][2]), s[1][2])
            target[q, 0] = jnp.where(keep1, jnp.where(even, s[0][1], down(s[1][1])), 0.0)
            target[q, 1] = jnp.where(even, s[0][2], down(s[1][2]))
            target[q, 2] = jnp.where(keep3, s[0][3], 0.0)
            target[q, 3] = jnp.where(keep3, s[1][3], 0.0)
            target[q, 4] = jnp.where(keep_mix, jnp.where(small, first, late), 0.0)

        lax.fori_loop(0, POINTS // 8, pack_points, 0)
        for q in (0, POINTS - 1):
            for v in range(PACK):
                target[q, v] = zero

        def weigh(block, carry):
            rows = pl.ds(block * PB, PB)
            pltpu.make_async_copy(inv_hbm.at[1, rows], later_v.at[rows], inv_sem.at[BLOCKS + block]).wait()
            weights = [[weight_ref[0, r, block * PB + p] for p in range(PB)] for r in range(2)]

            def tile_row(qb, carry):
                for b in range(4):
                    low, top = e_v[0, qb, b], e_v[1, qb, b]
                    for p in range(PB):
                        tile = later_v[block * PB + p, qb, :, b * LANES:(b + 1) * LANES]
                        low = low + weights[0][p] * tile
                        top = top + weights[1][p] * tile
                    e_v[0, qb, b] = low
                    e_v[1, qb, b] = top
                return carry

            return lax.fori_loop(0, POINTS // ROWS, tile_row, carry, unroll=2)

        def solve_and_weigh(block, carry):
            rows = pl.ds(block * PB, PB)
            pltpu.make_async_copy(inv_hbm.at[0, rows], inv_v.at[rows], inv_sem.at[block]).wait()

            @pl.when(block + AHEAD < BLOCKS)
            def _():
                ahead = pl.ds((block + AHEAD) * PB, PB)
                pltpu.make_async_copy(inv_hbm.at[0, ahead], inv_v.at[ahead], inv_sem.at[block + AHEAD]).start()

            @pl.when(block == 2)
            def _():
                sources[1].start()

            pltpu.make_async_copy(inv_hbm.at[1, rows], later_v.at[rows], inv_sem.at[BLOCKS + block]).start()
            solve_block(f, inv_v, first_v, block, small, odd_v, part_v)
            sums = list(carry)
            for p in range(PB):
                at = block * PB + p
                x = [part_v[f, at, v] for v in range(KEPT)]
                for r in range(2):
                    weight = weight_ref[0, r, at]
                    for v in range(KEPT):
                        sums[r * KEPT + v] = sums[r * KEPT + v] + weight * x[v]
            return tuple(sums)

        if f == 0:
            sums = lax.fori_loop(0, BLOCKS, solve_and_weigh, (zero,) * (2 * KEPT))
            for r in range(2):
                for v in range(PACK):
                    msg_ref[r * PACK + v] = sums[r * KEPT + v]
                msg_ref[2 * PACK + r] = sums[r * KEPT + PACK]
            continue
        for r in range(2):
            for qb in range(POINTS // ROWS):
                for b in range(4):
                    e_v[r, qb, b] = zero
        lax.fori_loop(0, BLOCKS, weigh, 0)

        def accumulate(qb, sums):
            sums = list(sums)
            for row in range(ROWS):
                x = [packed_v[qb * ROWS + row, v] for v in range(PACK)]
                for r in range(2):
                    e = [jnp.broadcast_to(e_v[r, qb, b, row:row + 1, :], (ROWS, LANES)) for b in range(4)]
                    e = [e[1], e[2], e[3], e[3], jnp.where(small, e[0], e[2])]
                    for v in range(PACK):
                        sums[r * PACK + v] = sums[r * PACK + v] + e[v] * x[v]
            return tuple(sums)

        sums = lax.fori_loop(0, POINTS // ROWS, accumulate, (zero,) * (2 * PACK))
        for i in range(2 * PACK):
            msg_ref[f * MESSAGE + i] = sums[i]
        for r in range(2):
            for b in range(4):
                msg_ref[f * MESSAGE + 2 * PACK + r, 2 * b:2 * b + 1, :] = e_v[r, 0, b, 0:1, :]
                msg_ref[f * MESSAGE + 2 * PACK + r, 2 * b + 1:2 * b + 2, :] = (
                    e_v[r, POINTS // ROWS - 1, b, ROWS - 1:ROWS, :]
                )


ANY = pl.BlockSpec(memory_space=pl.ANY)
SCALARS = pl.BlockSpec(memory_space=pltpu.SMEM)
INVERSE_V = pltpu.VMEM((POINTS, POINTS // ROWS, ROWS, 512), F32)
PACKED_V = pltpu.VMEM((POINTS, PACK, ROWS, LANES), F32)
MESSAGE_V = pltpu.VMEM((FIELDS * MESSAGE, ROWS, LANES), F32)
PART_V = pltpu.VMEM((FIELDS, POINTS, KEPT, ROWS, LANES), F32)
SENT_V = pltpu.VMEM((GROUPS, SENT, ROWS, LANES), F32)
IN_VMEM = pl.BlockSpec(memory_space=pltpu.VMEM)
IN_HBM = pl.BlockSpec(memory_space=pltpu.HBM)


def grant(mib):
    return pltpu.CompilerParams(vmem_limit_bytes=mib * 2**20)


def held(x):
    return pltpu.with_memory_space_constraint(x, pltpu.VMEM)


def far(x):
    return pltpu.with_memory_space_constraint(x, pltpu.HBM)


def dma(*shape):
    return pltpu.SemaphoreType.DMA(shape)


def slopes(slot, weights, inverse, forcing):
    return pl.pallas_call(
        slope_kernel,
        in_specs=[SCALARS, SCALARS, IN_HBM, IN_HBM],
        out_specs=[IN_VMEM] * 4,
        out_shape=[INVERSE_V, PACKED_V, MESSAGE_V, PART_V],
        scratch_shapes=[
            INVERSE_V,
            pltpu.VMEM((FIELDS, POINTS, 2, ROWS, 512), F32),
            PACKED_V,
            pltpu.VMEM((2, POINTS // ROWS, 4, ROWS, LANES), F32),
            pltpu.VMEM((3 * PB, ROWS, LANES), F32),
            dma(CHUNKS),
            dma(FIELDS),
        ],
        compiler_params=grant(SLOPES_MIB),
        cost_estimate=pl.CostEstimate(flops=20_000_000, bytes_accessed=24_000_000, transcendentals=0),
        name="slopes",
    )(far(slot), far(weights), far(inverse), far(forcing))


def block_sums(f, inv_v, packed_v, block, small, odd_v):
    zero = jnp.zeros((ROWS, LANES), F32)

    def unit(p, qb, r, b):
        line = inv_v[block * PB + p, qb, r:r + 1, b * LANES:(b + 1) * LANES]
        return jnp.broadcast_to(line, (ROWS, LANES))

    def odd_rows(qb, sums, rows):
        sums = list(sums)
        for r in rows:
            s = [packed_v[qb * ROWS + r, v] for v in (0, 2, 3)]
            for p in range(PB):
                one = unit(p, qb, r, 1)
                three = unit(p, qb, r, 3)
                sums[3 * p] = sums[3 * p] + one * s[0]
                sums[3 * p + 1] = sums[3 * p + 1] + three * s[1]
                sums[3 * p + 2] = sums[3 * p + 2] + three * s[2]
        return tuple(sums)

    def even_rows(qb, sums, rows):
        sums = list(sums)
        for r in rows:
            s = [packed_v[qb * ROWS + r, v] for v in (1, 4)]
            for p in range(PB):
                none = unit(p, qb, r, 0)
                two = unit(p, qb, r, 2)
                sums[2 * p] = sums[2 * p] + two * s[0]
                sums[2 * p + 1] = sums[2 * p + 1] + jnp.where(small, none, two) * s[1]
        return tuple(sums)

    def all_rows(rows_of, sums):
        last = POINTS // ROWS - 1
        sums = rows_of(0, sums, range(1, ROWS))
        sums = lax.fori_loop(1, last, lambda qb, c: rows_of(qb, c, range(ROWS)), sums)
        return rows_of(last, sums, range(ROWS - 1))

    odd = all_rows(odd_rows, (zero,) * (3 * PB))
    for i in range(3 * PB):
        odd_v[i] = odd[i]
    even = all_rows(even_rows, (zero,) * (2 * PB))
    return [[odd_v[3 * p], even[2 * p], odd_v[3 * p + 1], odd_v[3 * p + 2], even[2 * p + 1]] for p in range(PB)]


def solve_block(f, inv_v, packed_v, block, small, odd_v, part_v):
    x = block_sums(f, inv_v, packed_v, block, small, odd_v)
    for p in range(PB):
        at = block * PB + p
        for v in range(PACK):
            part_v[f, at, v] = x[p][v]
        for b in range(4):
            lanes = slice(b * LANES, (b + 1) * LANES)
            part_v[f, at, PACK, 2 * b:2 * b + 1, :] = inv_v[at, 0, 0:1, lanes]
            part_v[f, at, PACK, 2 * b + 1:2 * b + 2, :] = inv_v[at, POINTS // ROWS - 1, ROWS - 1:ROWS, lanes]


def particular_kernel(slot_ref, inv_v, packed_v, early_v, part_v, odd_v):
    small = pair_wavenumber(slot_ref) < LANES

    def step(block, carry):
        solve_block(FIELDS - 1, inv_v, packed_v, block, small, odd_v, part_v)
        return carry

    lax.fori_loop(0, BLOCKS, step, 0)


def particular(slot, inverse, packed, early):
    return pl.pallas_call(
        particular_kernel,
        in_specs=[SCALARS] + [IN_VMEM] * 3,
        out_specs=IN_VMEM,
        out_shape=PART_V,
        input_output_aliases={3: 0},
        scratch_shapes=[pltpu.VMEM((3 * PB, ROWS, LANES), F32)],
        compiler_params=grant(PARTICULAR_MIB),
        cost_estimate=pl.CostEstimate(flops=90_000_000, bytes_accessed=24_000_000, transcendentals=0),
        name="particular",
    )(far(slot), held(inverse), held(packed), held(early))


def solve_interface(f, all_v, u_v, small):
    base = f * MESSAGE
    zero = jnp.zeros((ROWS, LANES), F32)
    for v in range(PACK):
        u_v[0, f, v] = zero
        u_v[NSUB, f, v] = zero

    def coefficient(t, r, k, b):
        return all_v[t, base + 2 * PACK + r, pl.ds(2 * b + k, ROWS, stride=0), :]

    ratio = [zero] * PACK
    reduced = [zero] * PACK
    ratios = []
    reduceds = []
    for level in range(NSUB - 1):
        factors = []
        for b in range(4):
            lower = coefficient(level, 1, 0, b)
            middle = coefficient(level, 1, 1, b) - coefficient(level + 1, 0, 0, b)
            upper = -coefficient(level + 1, 0, 1, b)
            factors.append((lower, middle, upper))
        mixed = tuple(jnp.where(small, x, y) for x, y in zip(factors[0], factors[2]))
        new_ratio, new_reduced = [None] * PACK, [None] * PACK
        for v, (lower, middle, upper) in enumerate((factors[1], factors[2], factors[3], factors[3], mixed)):
            right = all_v[level + 1, base + v] - all_v[level, base + PACK + v]
            inverted = last if v == 3 else 1.0 / (middle - lower * ratio[v])
            last = inverted
            new_ratio[v] = upper * inverted
            new_reduced[v] = (right - lower * reduced[v]) * inverted
        ratio, reduced = new_ratio, new_reduced
        ratios.append(ratio)
        reduceds.append(reduced)
    later = [zero] * PACK
    for level in range(NSUB - 2, -1, -1):
        later = [reduceds[level][v] - ratios[level][v] * later[v] for v in range(PACK)]
        for v in range(PACK):
            u_v[level + 1, f, v] = later[v]


PER = PB // NEAR


def pack_kernel(slot_ref, *refs):
    blocks = refs[:NSUB]
    part_v, out_v, all_v, u_v = refs[NSUB:]
    sub = lax.axis_index("sub")
    level, core = sub // 2, lax.rem(sub, 2)
    for k in range(NSUB):
        other, turn = k // 4, k % 4
        place = lax.rem(level + (4 - turn), 4) * 2 + (core if other == 0 else 1 - core)
        for i in range(FIELDS * MESSAGE):
            all_v[place, i] = blocks[k][i]
    m = pair_wavenumber(slot_ref)
    lane = lane_iota()
    even = row_iota() % 2 == 0
    small = m < LANES
    for f in range(FIELDS):
        solve_interface(f, all_v, u_v, small)

    def step(block, carry):
        for d in range(PER):
            dest = block * PER + d
            extra = jnp.where(lane == FIELDS * NEAR, m.astype(F32), 0.0)
            for f in range(FIELDS):
                u_low = [u_v[sub, f, v] for v in range(PACK)]
                u_top = [u_v[sub + 1, f, v] for v in range(PACK)]
                for k in range(NEAR):
                    p = block * PB + d * NEAR + k
                    low = [part_v[f, p, PACK, pl.ds(2 * b, ROWS, stride=0), :] for b in range(4)]
                    top = [part_v[f, p, PACK, pl.ds(2 * b + 1, ROWS, stride=0), :] for b in range(4)]
                    low = [low[1], low[2], low[3], low[3], jnp.where(small, low[0], low[2])]
                    top = [top[1], top[2], top[3], top[3], jnp.where(small, top[0], top[2])]
                    x = [part_v[f, p, v] + u_low[v] * low[v] + u_top[v] * top[v] for v in range(PACK)]
                    s, spare = fold(x, m, lane, even, small)
                    at = f * NEAR + k
                    for b in range(4):
                        out_v[dest, at * 4 + b] = s[b]
                    extra = jnp.where(lane == at, spare, extra)
            out_v[dest, SENT - 1] = extra
        return carry

    lax.fori_loop(0, BLOCKS, step, 0)


def pack(slot, messages, part):
    return pl.pallas_call(
        pack_kernel,
        in_specs=[SCALARS] + [IN_VMEM] * (NSUB + 1),
        out_specs=IN_VMEM,
        out_shape=SENT_V,
        scratch_shapes=[
            pltpu.VMEM((NSUB, FIELDS * MESSAGE, ROWS, LANES), F32),
            pltpu.VMEM((NSUB + 1, FIELDS, PACK, ROWS, LANES), F32),
        ],
        compiler_params=grant(PACK_MIB),
        name="pack",
    )(far(slot), *[held(x) for x in messages], held(part))


STEPS = 8
FROM = GROUPS // STEPS


def unpack_kernel(in_v, out_hbm, out_v, out_sem):
    def out_copy(i):
        rows = pl.ds(pl.multiple_of(i * FROM * ROWS, ROWS), FROM * ROWS)
        return pltpu.make_async_copy(out_v.at[:, :, :, rows, :], out_hbm.at[:, :, :, rows, :], out_sem.at[i])

    lane = lane_iota()
    even = row_iota() % 2 == 0

    def step(i, carry):
        for d in range(FROM):
            g = i * FROM + d
            extras = in_v[g, SENT - 1]
            m = column(extras, FIELDS * NEAR).astype(jnp.int32)
            small = m < LANES
            rows = pl.ds(pl.multiple_of(g * ROWS, ROWS), ROWS)
            for f in range(FIELDS):
                for k in range(NEAR):
                    at = f * NEAR + k
                    s = [in_v[g, at * 4 + b] for b in range(4)]
                    tiles = unfold(s, column(extras, at), m, lane, even, small)
                    for c in range(2):
                        for b in range(4):
                            out_v[f, k, c, rows, b * LANES:(b + 1) * LANES] = tiles[c][b]
        out_copy(i).start()
        return carry

    lax.fori_loop(0, STEPS, step, 0)
    wait_all(out_copy, STEPS)


def unpack(received):
    return pl.pallas_call(
        unpack_kernel,
        in_specs=[IN_VMEM],
        out_specs=ANY,
        out_shape=jax.ShapeDtypeStruct((FIELDS, NEAR, 2, GROUPS * ROWS, 512), F32),
        scratch_shapes=[pltpu.VMEM((FIELDS, NEAR, 2, GROUPS * ROWS, 512), F32), dma(STEPS)],
        compiler_params=grant(UNPACK_MIB),
        name="unpack",
    )(held(received))


def over_ma(sent):
    flat = sent.reshape(GROUPS, SENT * ROWS, LANES)
    received = lax.all_to_all(flat, "ma", split_axis=0, concat_axis=0, tiled=True)
    return received.reshape(GROUPS, SENT, ROWS, LANES)


def body(forcing, slot_wavenumber, inverse, edge_weights):
    inverse = inverse.reshape(FIELDS, POINTS, POINTS // ROWS, ROWS, 512)
    later, packed, message, early = slopes(slot_wavenumber, edge_weights, inverse, forcing)
    column = [message]
    for k in range(1, 4):
        column.append(lax.ppermute(message, "sub", [(i, (i + 2 * k) % NSUB) for i in range(NSUB)]))
    part = particular(slot_wavenumber, later, packed, early)
    partner = [(i, i ^ 1) for i in range(NSUB)]
    twin = [lax.ppermute(message, "sub", partner)]
    part, *column[1:] = lax.optimization_barrier((part, *column[1:]))
    messages = column + twin + [lax.ppermute(x, "sub", partner) for x in column[1:]]
    sent = pack(slot_wavenumber, messages, part)
    return unpack(over_ma(sent))


def solution(mesh):
    return jax.shard_map(
        body,
        mesh=mesh,
        in_specs=(
            P(None, "sub", None, "ma", None),
            P("ma"),
            P("sub", None, None, None, None),
            P("sub", None, None),
        ),
        out_specs=P(None, ("sub", "ma"), None, None, None),
        check_vma=False,
    )
```

```python
import jax
import jax.numpy as jnp
from jax import lax
from jax.experimental import pallas as pl
from jax.experimental.pallas import tpu as pltpu
from jax.sharding import PartitionSpec as P

F32 = jnp.float32
POINTS = 64
FIELDS = 2
NSUB = 8
GROUPS = 16
LANES = 128
ROWS = 8
PACK = 5
QB = 8
PB = 8
NEAR = POINTS // GROUPS
SENT = FIELDS * NEAR * 4 + 1
MESSAGE = 2 * PACK + 2
BLOCKS = POINTS // PB


def lane_iota():
    return lax.broadcasted_iota(jnp.int32, (ROWS, LANES), 1)


def row_iota():
    return lax.broadcasted_iota(jnp.int32, (ROWS, LANES), 0)


def pair_wavenumber(slot_ref):
    pair = row_iota() // 2
    m = jnp.full((ROWS, LANES), slot_ref[0], jnp.int32)
    for j in range(1, 4):
        m = jnp.where(pair == j, slot_ref[2 * j], m)
    return m


def down(x):
    return pltpu.roll(x, 1, 0)


def up(x):
    return pltpu.roll(x, ROWS - 1, 0)


def fold(x, m, lane, even, small):
    shift = jnp.where(small, m, m - LANES)
    turn = (lane - shift + LANES) % LANES
    below = lane < shift
    low3 = jnp.where(even, x[2], down(x[3]))
    high3 = jnp.where(even, up(x[2]), x[3])
    high3_t = jnp.take_along_axis(high3, turn, axis=1)
    mix_t = jnp.take_along_axis(x[4], turn, axis=1)
    zero = jnp.where(small, jnp.where(below, high3_t, x[4]), jnp.where(below, mix_t, high3_t))
    one = jnp.where(jnp.logical_and(below, jnp.logical_not(small)), high3_t, x[0])
    last = jnp.full((ROWS, LANES), LANES - 1, jnp.int32)
    spare = jnp.take_along_axis(jnp.where(small, high3_t, mix_t), last, axis=1)
    return (zero, one, x[1], low3), spare


def column(x, k):
    return jnp.take_along_axis(x, jnp.full((ROWS, LANES), k, jnp.int32), axis=1)


def unfold(s, spare, m, lane, even, small):
    shift = jnp.where(small, m, m - LANES)
    back = (lane + shift) % LANES
    after = lane >= LANES - shift
    exact = lane == LANES - 1 - shift
    g0 = jnp.take_along_axis(s[0], back, axis=1)
    g1 = jnp.take_along_axis(s[1], back, axis=1)
    value = jnp.where(after, g0, jnp.where(exact, spare, 0.0))
    high3 = jnp.where(small, value, jnp.where(after, g1, g0))
    high2 = jnp.where(small, 0.0, value)
    low0 = jnp.where(lane >= m, s[0], 0.0)
    low1 = jnp.where(lane + LANES >= m, s[1], 0.0)
    lows = [low0, low1, s[2], s[3]]
    first = [jnp.where(even, low0, 0.0), jnp.where(even, low1, 0.0)]
    first += [jnp.where(even, s[2], down(high2)), jnp.where(even, s[3], down(high3))]
    second = [jnp.where(even, up(low0), 0.0), jnp.where(even, up(low1), 0.0)]
    second += [jnp.where(even, up(s[2]), high2), jnp.where(even, up(s[3]), high3)]
    return first, second


AHEAD = 3
SLOPES_MIB = 18
PARTICULAR_MIB = 4
PACK_MIB = 4
UNPACK_MIB = 8
KEPT = PACK + 1
CHUNKS = FIELDS * BLOCKS


def inverse_chunks(inv_hbm, held_v, sem):
    def copy(i):
        f, block = i // BLOCKS, i % BLOCKS
        rows = pl.ds(block * PB, PB)
        return pltpu.make_async_copy(inv_hbm.at[f, rows], held_v[f].at[rows], sem.at[i])

    return copy


def wait_all(copy, count, first=0):
    def step(i, carry):
        copy(i).wait()
        return carry

    lax.fori_loop(first, count, step, 0)


def slope_kernel(
    slot_hbm, weight_hbm, inv_hbm, src_hbm, later_v, packed_v, msg_ref, part_v, m_ref,
    inv_v, src_v, first_v, e_v, odd_v, slot_ref, weight_ref, inv_sem, src_sem, scalar_sem
):
    copy = inverse_chunks(inv_hbm, (inv_v, later_v), inv_sem)
    sources = [pltpu.make_async_copy(src_hbm.at[f], src_v.at[f], src_sem.at[f]) for f in range(FIELDS)]

    scalars = [
        pltpu.make_async_copy(slot_hbm, slot_ref, scalar_sem.at[0]),
        pltpu.make_async_copy(weight_hbm, weight_ref, scalar_sem.at[1]),
    ]
    scalars[0].start()
    sources[0].start()
    copy(0).start()
    scalars[1].start()
    for scalar in scalars:
        scalar.wait()
    m = pair_wavenumber(slot_ref)
    m_ref[...] = m
    lane = lane_iota()
    even = row_iota() % 2 == 0
    small = m < LANES
    zero = jnp.zeros((ROWS, LANES), F32)
    keep1 = lane + LANES >= m
    keep3 = lane + 3 * LANES >= jnp.where(even, m, 511 - m)
    keep_mix = lane >= jnp.where(small, m, 255 - m)
    for f in range(FIELDS):
        sources[f].wait()
        if f == 0:
            for i in range(1, AHEAD):
                copy(i).start()

        target = first_v if f == 0 else packed_v

        def pack_points(i, carry):
            for k in range(8):
                pack_point(i * 8 + k)
            return carry

        def pack_point(q):
            s = [[src_v[f, q, c, :, b * LANES:(b + 1) * LANES] for b in range(4)] for c in range(2)]
            first = jnp.where(even, s[0][0], down(s[1][0]))
            late = jnp.where(even, up(s[0][2]), s[1][2])
            target[q, 0] = jnp.where(keep1, jnp.where(even, s[0][1], down(s[1][1])), 0.0)
            target[q, 1] = jnp.where(even, s[0][2], down(s[1][2]))
            target[q, 2] = jnp.where(keep3, s[0][3], 0.0)
            target[q, 3] = jnp.where(keep3, s[1][3], 0.0)
            target[q, 4] = jnp.where(keep_mix, jnp.where(small, first, late), 0.0)

        lax.fori_loop(0, POINTS // 8, pack_points, 0)
        for q in (0, POINTS - 1):
            for v in range(PACK):
                target[q, v] = zero

        def weigh(block, carry):
            rows = pl.ds(block * PB, PB)
            pltpu.make_async_copy(inv_hbm.at[1, rows], later_v.at[rows], inv_sem.at[BLOCKS + block]).wait()
            weights = [[weight_ref[0, r, block * PB + p] for p in range(PB)] for r in range(2)]

            def tile_row(qb, carry):
                for b in range(4):
                    low, top = e_v[0, qb, b], e_v[1, qb, b]
                    for p in range(PB):
                        tile = later_v[block * PB + p, qb, :, b * LANES:(b + 1) * LANES]
                        low = low + weights[0][p] * tile
                        top = top + weights[1][p] * tile
                    e_v[0, qb, b] = low
                    e_v[1, qb, b] = top
                return carry

            return lax.fori_loop(0, POINTS // ROWS, tile_row, carry, unroll=2)

        def solve_and_weigh(block, carry):
            rows = pl.ds(block * PB, PB)
            pltpu.make_async_copy(inv_hbm.at[0, rows], inv_v.at[rows], inv_sem.at[block]).wait()

            @pl.when(block + AHEAD < BLOCKS)
            def _():
                ahead = pl.ds((block + AHEAD) * PB, PB)
                pltpu.make_async_copy(inv_hbm.at[0, ahead], inv_v.at[ahead], inv_sem.at[block + AHEAD]).start()

            @pl.when(block == 2)
            def _():
                sources[1].start()

            pltpu.make_async_copy(inv_hbm.at[1, rows], later_v.at[rows], inv_sem.at[BLOCKS + block]).start()
            solve_block(f, inv_v, first_v, block, small, odd_v, part_v)
            sums = list(carry)
            for p in range(PB):
                at = block * PB + p
                x = [part_v[f, at, v] for v in range(KEPT)]
                for r in range(2):
                    weight = weight_ref[0, r, at]
                    for v in range(KEPT):
                        sums[r * KEPT + v] = sums[r * KEPT + v] + weight * x[v]
            return tuple(sums)

        if f == 0:
            sums = lax.fori_loop(0, BLOCKS, solve_and_weigh, (zero,) * (2 * KEPT))
            for r in range(2):
                for v in range(PACK):
                    msg_ref[r * PACK + v] = sums[r * KEPT + v]
                msg_ref[2 * PACK + r] = sums[r * KEPT + PACK]
            continue
        for r in range(2):
            for qb in range(POINTS // ROWS):
                for b in range(4):
                    e_v[r, qb, b] = zero
        lax.fori_loop(0, BLOCKS, weigh, 0)

        def accumulate(qb, sums):
            sums = list(sums)
            for row in range(ROWS):
                x = [packed_v[qb * ROWS + row, v] for v in range(PACK)]
                for r in range(2):
                    e = [jnp.broadcast_to(e_v[r, qb, b, row:row + 1, :], (ROWS, LANES)) for b in range(4)]
                    e = [e[1], e[2], e[3], e[3], jnp.where(small, e[0], e[2])]
                    for v in range(PACK):
                        sums[r * PACK + v] = sums[r * PACK + v] + e[v] * x[v]
            return tuple(sums)

        sums = lax.fori_loop(0, POINTS // ROWS, accumulate, (zero,) * (2 * PACK))
        for i in range(2 * PACK):
            msg_ref[f * MESSAGE + i] = sums[i]
        for r in range(2):
            for b in range(4):
                msg_ref[f * MESSAGE + 2 * PACK + r, 2 * b:2 * b + 1, :] = e_v[r, 0, b, 0:1, :]
                msg_ref[f * MESSAGE + 2 * PACK + r, 2 * b + 1:2 * b + 2, :] = (
                    e_v[r, POINTS // ROWS - 1, b, ROWS - 1:ROWS, :]
                )


ANY = pl.BlockSpec(memory_space=pl.ANY)
INVERSE_V = pltpu.VMEM((POINTS, POINTS // ROWS, ROWS, 512), F32)
PACKED_V = pltpu.VMEM((POINTS, PACK, ROWS, LANES), F32)
MESSAGE_V = pltpu.VMEM((FIELDS * MESSAGE, ROWS, LANES), F32)
PART_V = pltpu.VMEM((FIELDS, POINTS, KEPT, ROWS, LANES), F32)
SENT_V = pltpu.VMEM((GROUPS, SENT, ROWS, LANES), F32)
IN_VMEM = pl.BlockSpec(memory_space=pltpu.VMEM)
IN_HBM = pl.BlockSpec(memory_space=pltpu.HBM)


def grant(mib):
    return pltpu.CompilerParams(vmem_limit_bytes=mib * 2**20)


def held(x):
    return pltpu.with_memory_space_constraint(x, pltpu.VMEM)


def far(x):
    return pltpu.with_memory_space_constraint(x, pltpu.HBM)


def dma(*shape):
    return pltpu.SemaphoreType.DMA(shape)


def slopes(slot, weights, inverse, forcing):
    return pl.pallas_call(
        slope_kernel,
        in_specs=[IN_HBM] * 4,
        out_specs=[IN_VMEM] * 5,
        out_shape=[INVERSE_V, PACKED_V, MESSAGE_V, PART_V, pltpu.VMEM((ROWS, LANES), jnp.int32)],
        scratch_shapes=[
            INVERSE_V,
            pltpu.VMEM((FIELDS, POINTS, 2, ROWS, 512), F32),
            PACKED_V,
            pltpu.VMEM((2, POINTS // ROWS, 4, ROWS, LANES), F32),
            pltpu.VMEM((3 * PB, ROWS, LANES), F32),
            pltpu.SMEM((ROWS,), jnp.int32),
            pltpu.SMEM((1, 2, POINTS), F32),
            dma(CHUNKS),
            dma(FIELDS),
            dma(2),
        ],
        compiler_params=grant(SLOPES_MIB),
        cost_estimate=pl.CostEstimate(flops=20_000_000, bytes_accessed=24_000_000, transcendentals=0),
        name="slopes",
    )(far(slot), far(weights), far(inverse), far(forcing))


def block_sums(f, inv_v, packed_v, block, small, odd_v):
    zero = jnp.zeros((ROWS, LANES), F32)

    def unit(p, qb, r, b):
        line = inv_v[block * PB + p, qb, r:r + 1, b * LANES:(b + 1) * LANES]
        return jnp.broadcast_to(line, (ROWS, LANES))

    def odd_rows(qb, sums, rows):
        sums = list(sums)
        for r in rows:
            s = [packed_v[qb * ROWS + r, v] for v in (0, 2, 3)]
            for p in range(PB):
                one = unit(p, qb, r, 1)
                three = unit(p, qb, r, 3)
                sums[3 * p] = sums[3 * p] + one * s[0]
                sums[3 * p + 1] = sums[3 * p + 1] + three * s[1]
                sums[3 * p + 2] = sums[3 * p + 2] + three * s[2]
        return tuple(sums)

    def even_rows(qb, sums, rows):
        sums = list(sums)
        for r in rows:
            s = [packed_v[qb * ROWS + r, v] for v in (1, 4)]
            for p in range(PB):
                none = unit(p, qb, r, 0)
                two = unit(p, qb, r, 2)
                sums[2 * p] = sums[2 * p] + two * s[0]
                sums[2 * p + 1] = sums[2 * p + 1] + jnp.where(small, none, two) * s[1]
        return tuple(sums)

    def all_rows(rows_of, sums):
        last = POINTS // ROWS - 1
        sums = rows_of(0, sums, range(1, ROWS))
        sums = lax.fori_loop(1, last, lambda qb, c: rows_of(qb, c, range(ROWS)), sums, unroll=2)
        return rows_of(last, sums, range(ROWS - 1))

    odd = all_rows(odd_rows, (zero,) * (3 * PB))
    for i in range(3 * PB):
        odd_v[i] = odd[i]
    even = all_rows(even_rows, (zero,) * (2 * PB))
    return [[odd_v[3 * p], even[2 * p], odd_v[3 * p + 1], odd_v[3 * p + 2], even[2 * p + 1]] for p in range(PB)]


def solve_block(f, inv_v, packed_v, block, small, odd_v, part_v):
    x = block_sums(f, inv_v, packed_v, block, small, odd_v)
    for p in range(PB):
        at = block * PB + p
        for v in range(PACK):
            part_v[f, at, v] = x[p][v]
        for b in range(4):
            lanes = slice(b * LANES, (b + 1) * LANES)
            part_v[f, at, PACK, 2 * b:2 * b + 1, :] = inv_v[at, 0, 0:1, lanes]
            part_v[f, at, PACK, 2 * b + 1:2 * b + 2, :] = inv_v[at, POINTS // ROWS - 1, ROWS - 1:ROWS, lanes]


def particular_kernel(m_ref, inv_v, packed_v, early_v, part_v, odd_v):
    small = m_ref[...] < LANES

    def step(block, carry):
        solve_block(FIELDS - 1, inv_v, packed_v, block, small, odd_v, part_v)
        return carry

    lax.fori_loop(0, BLOCKS, step, 0)


def particular(m, inverse, packed, early):
    return pl.pallas_call(
        particular_kernel,
        in_specs=[IN_VMEM] * 4,
        out_specs=IN_VMEM,
        out_shape=PART_V,
        input_output_aliases={3: 0},
        scratch_shapes=[pltpu.VMEM((3 * PB, ROWS, LANES), F32)],
        compiler_params=grant(PARTICULAR_MIB),
        cost_estimate=pl.CostEstimate(flops=90_000_000, bytes_accessed=24_000_000, transcendentals=0),
        name="particular",
    )(held(m), held(inverse), held(packed), held(early))


def solve_interface(f, all_v, u_v, small):
    base = f * MESSAGE
    zero = jnp.zeros((ROWS, LANES), F32)
    for v in range(PACK):
        u_v[0, f, v] = zero
        u_v[NSUB, f, v] = zero

    def coefficient(t, r, k, b):
        return all_v[t, base + 2 * PACK + r, pl.ds(2 * b + k, ROWS, stride=0), :]

    ratio = [zero] * PACK
    reduced = [zero] * PACK
    ratios = []
    reduceds = []
    for level in range(NSUB - 1):
        factors = []
        for b in range(4):
            lower = coefficient(level, 1, 0, b)
            middle = coefficient(level, 1, 1, b) - coefficient(level + 1, 0, 0, b)
            upper = -coefficient(level + 1, 0, 1, b)
            factors.append((lower, middle, upper))
        mixed = tuple(jnp.where(small, x, y) for x, y in zip(factors[0], factors[2]))
        new_ratio, new_reduced = [None] * PACK, [None] * PACK
        for v, (lower, middle, upper) in enumerate((factors[1], factors[2], factors[3], factors[3], mixed)):
            right = all_v[level + 1, base + v] - all_v[level, base + PACK + v]
            inverted = last if v == 3 else 1.0 / (middle - lower * ratio[v])
            last = inverted
            new_ratio[v] = upper * inverted
            new_reduced[v] = (right - lower * reduced[v]) * inverted
        ratio, reduced = new_ratio, new_reduced
        ratios.append(ratio)
        reduceds.append(reduced)
    later = [zero] * PACK
    for level in range(NSUB - 2, -1, -1):
        later = [reduceds[level][v] - ratios[level][v] * later[v] for v in range(PACK)]
        for v in range(PACK):
            u_v[level + 1, f, v] = later[v]


PER = PB // NEAR


def pack_kernel(m_ref, *refs):
    blocks = refs[:NSUB]
    part_v, out_v, all_v, u_v = refs[NSUB:]
    sub = lax.axis_index("sub")
    level, core = sub // 2, lax.rem(sub, 2)
    for k in range(NSUB):
        other, turn = k // 4, k % 4
        place = lax.rem(level + (4 - turn), 4) * 2 + (core if other == 0 else 1 - core)
        for i in range(FIELDS * MESSAGE):
            all_v[place, i] = blocks[k][i]
    m = m_ref[...]
    lane = lane_iota()
    even = row_iota() % 2 == 0
    small = m < LANES
    for f in range(FIELDS):
        solve_interface(f, all_v, u_v, small)

    def step(block, carry):
        for d in range(PER):
            dest = block * PER + d
            extra = jnp.where(lane == FIELDS * NEAR, m.astype(F32), 0.0)
            for f in range(FIELDS):
                u_low = [u_v[sub, f, v] for v in range(PACK)]
                u_top = [u_v[sub + 1, f, v] for v in range(PACK)]
                for k in range(NEAR):
                    p = block * PB + d * NEAR + k
                    low = [part_v[f, p, PACK, pl.ds(2 * b, ROWS, stride=0), :] for b in range(4)]
                    top = [part_v[f, p, PACK, pl.ds(2 * b + 1, ROWS, stride=0), :] for b in range(4)]
                    low = [low[1], low[2], low[3], low[3], jnp.where(small, low[0], low[2])]
                    top = [top[1], top[2], top[3], top[3], jnp.where(small, top[0], top[2])]
                    x = [part_v[f, p, v] + u_low[v] * low[v] + u_top[v] * top[v] for v in range(PACK)]
                    s, spare = fold(x, m, lane, even, small)
                    at = f * NEAR + k
                    for b in range(4):
                        out_v[dest, at * 4 + b] = s[b]
                    extra = jnp.where(lane == at, spare, extra)
            out_v[dest, SENT - 1] = extra
        return carry

    lax.fori_loop(0, BLOCKS, step, 0)


def pack(m, messages, part):
    return pl.pallas_call(
        pack_kernel,
        in_specs=[IN_VMEM] * (NSUB + 2),
        out_specs=IN_VMEM,
        out_shape=SENT_V,
        scratch_shapes=[
            pltpu.VMEM((NSUB, FIELDS * MESSAGE, ROWS, LANES), F32),
            pltpu.VMEM((NSUB + 1, FIELDS, PACK, ROWS, LANES), F32),
        ],
        compiler_params=grant(PACK_MIB),
        name="pack",
    )(held(m), *[held(x) for x in messages], held(part))


STEPS = 8
FROM = GROUPS // STEPS


def unpack_kernel(in_v, out_hbm, out_v, out_sem):
    def out_copy(i):
        rows = pl.ds(pl.multiple_of(i * FROM * ROWS, ROWS), FROM * ROWS)
        return pltpu.make_async_copy(out_v.at[:, :, :, rows, :], out_hbm.at[:, :, :, rows, :], out_sem.at[i])

    lane = lane_iota()
    even = row_iota() % 2 == 0

    def step(i, carry):
        for d in range(FROM):
            g = i * FROM + d
            extras = in_v[g, SENT - 1]
            m = column(extras, FIELDS * NEAR).astype(jnp.int32)
            small = m < LANES
            rows = pl.ds(pl.multiple_of(g * ROWS, ROWS), ROWS)
            for f in range(FIELDS):
                for k in range(NEAR):
                    at = f * NEAR + k
                    s = [in_v[g, at * 4 + b] for b in range(4)]
                    tiles = unfold(s, column(extras, at), m, lane, even, small)
                    for c in range(2):
                        for b in range(4):
                            out_v[f, k, c, rows, b * LANES:(b + 1) * LANES] = tiles[c][b]
        out_copy(i).start()
        return carry

    lax.fori_loop(0, STEPS, step, 0)
    wait_all(out_copy, STEPS)


def unpack(received):
    return pl.pallas_call(
        unpack_kernel,
        in_specs=[IN_VMEM],
        out_specs=ANY,
        out_shape=jax.ShapeDtypeStruct((FIELDS, NEAR, 2, GROUPS * ROWS, 512), F32),
        scratch_shapes=[pltpu.VMEM((FIELDS, NEAR, 2, GROUPS * ROWS, 512), F32), dma(STEPS)],
        compiler_params=grant(UNPACK_MIB),
        name="unpack",
    )(held(received))


def over_ma(sent):
    flat = sent.reshape(GROUPS, SENT * ROWS, LANES)
    received = lax.all_to_all(flat, "ma", split_axis=0, concat_axis=0, tiled=True)
    return received.reshape(GROUPS, SENT, ROWS, LANES)


def body(forcing, slot_wavenumber, inverse, edge_weights):
    inverse = inverse.reshape(FIELDS, POINTS, POINTS // ROWS, ROWS, 512)
    later, packed, message, early, m = slopes(slot_wavenumber, edge_weights, inverse, forcing)
    column = [message]
    for k in range(1, 4):
        column.append(lax.ppermute(message, "sub", [(i, (i + 2 * k) % NSUB) for i in range(NSUB)]))
    part = particular(m, later, packed, early)
    partner = [(i, i ^ 1) for i in range(NSUB)]
    twin = [lax.ppermute(message, "sub", partner)]
    part, *column[1:] = lax.optimization_barrier((part, *column[1:]))
    messages = column + twin + [lax.ppermute(x, "sub", partner) for x in column[1:]]
    sent = pack(m, messages, part)
    return unpack(over_ma(sent))


def solution(mesh):
    return jax.shard_map(
        body,
        mesh=mesh,
        in_specs=(
            P(None, "sub", None, "ma", None),
            P("ma"),
            P("sub", None, None, None, None),
            P("sub", None, None),
        ),
        out_specs=P(None, ("sub", "ma"), None, None, None),
        check_vma=False,
    )
```

```python
import jax
import jax.numpy as jnp
from jax import lax
from jax.experimental import pallas as pl
from jax.experimental.pallas import tpu as pltpu
from jax.sharding import PartitionSpec as P

F32 = jnp.float32
POINTS = 64
FIELDS = 2
NSUB = 8
GROUPS = 16
LANES = 128
ROWS = 8
PACK = 5
QB = 8
PB = 8
NEAR = POINTS // GROUPS
SENT = FIELDS * NEAR * 4 + 1
MESSAGE = 2 * PACK + 2
BLOCKS = POINTS // PB


def lane_iota():
    return lax.broadcasted_iota(jnp.int32, (ROWS, LANES), 1)


def row_iota():
    return lax.broadcasted_iota(jnp.int32, (ROWS, LANES), 0)


def pair_wavenumber(slot_ref):
    pair = row_iota() // 2
    m = jnp.full((ROWS, LANES), slot_ref[0], jnp.int32)
    for j in range(1, 4):
        m = jnp.where(pair == j, slot_ref[2 * j], m)
    return m


def down(x):
    return pltpu.roll(x, 1, 0)


def up(x):
    return pltpu.roll(x, ROWS - 1, 0)


def fold(x, m, lane, even, small):
    shift = jnp.where(small, m, m - LANES)
    turn = (lane - shift + LANES) % LANES
    below = lane < shift
    low3 = jnp.where(even, x[2], down(x[3]))
    high3 = jnp.where(even, up(x[2]), x[3])
    high3_t = jnp.take_along_axis(high3, turn, axis=1)
    mix_t = jnp.take_along_axis(x[4], turn, axis=1)
    zero = jnp.where(small, jnp.where(below, high3_t, x[4]), jnp.where(below, mix_t, high3_t))
    one = jnp.where(jnp.logical_and(below, jnp.logical_not(small)), high3_t, x[0])
    last = jnp.full((ROWS, LANES), LANES - 1, jnp.int32)
    spare = jnp.take_along_axis(jnp.where(small, high3_t, mix_t), last, axis=1)
    return (zero, one, x[1], low3), spare


def column(x, k):
    return jnp.take_along_axis(x, jnp.full((ROWS, LANES), k, jnp.int32), axis=1)


def unfold(s, spare, m, lane, even, small):
    shift = jnp.where(small, m, m - LANES)
    back = (lane + shift) % LANES
    after = lane >= LANES - shift
    exact = lane == LANES - 1 - shift
    g0 = jnp.take_along_axis(s[0], back, axis=1)
    g1 = jnp.take_along_axis(s[1], back, axis=1)
    value = jnp.where(after, g0, jnp.where(exact, spare, 0.0))
    high3 = jnp.where(small, value, jnp.where(after, g1, g0))
    high2 = jnp.where(small, 0.0, value)
    low0 = jnp.where(lane >= m, s[0], 0.0)
    low1 = jnp.where(lane + LANES >= m, s[1], 0.0)
    lows = [low0, low1, s[2], s[3]]
    first = [jnp.where(even, low0, 0.0), jnp.where(even, low1, 0.0)]
    first += [jnp.where(even, s[2], down(high2)), jnp.where(even, s[3], down(high3))]
    second = [jnp.where(even, up(low0), 0.0), jnp.where(even, up(low1), 0.0)]
    second += [jnp.where(even, up(s[2]), high2), jnp.where(even, up(s[3]), high3)]
    return first, second


AHEAD = 3
SLOPES_MIB = 18
PARTICULAR_MIB = 4
PACK_MIB = 4
UNPACK_MIB = 8
KEPT = PACK + 1
CHUNKS = FIELDS * BLOCKS


def inverse_chunks(inv_hbm, held_v, sem):
    def copy(i):
        f, block = i // BLOCKS, i % BLOCKS
        rows = pl.ds(block * PB, PB)
        return pltpu.make_async_copy(inv_hbm.at[f, rows], held_v[f].at[rows], sem.at[i])

    return copy


def wait_all(copy, count, first=0):
    def step(i, carry):
        copy(i).wait()
        return carry

    lax.fori_loop(first, count, step, 0)


def slope_kernel(
    slot_hbm, weight_hbm, inv_hbm, src_hbm, later_v, packed_v, msg_ref, part_v, m_ref,
    inv_v, src_v, first_v, e_v, odd_v, slot_ref, weight_ref, inv_sem, src_sem, scalar_sem
):
    copy = inverse_chunks(inv_hbm, (inv_v, later_v), inv_sem)
    def source(f, half):
        rows = pl.ds(half * (POINTS // 2), POINTS // 2)
        return pltpu.make_async_copy(src_hbm.at[f, rows], src_v.at[f, rows], src_sem.at[2 * f + half])


    scalars = [
        pltpu.make_async_copy(slot_hbm, slot_ref, scalar_sem.at[0]),
        pltpu.make_async_copy(weight_hbm, weight_ref, scalar_sem.at[1]),
    ]
    scalars[0].start()
    source(0, 0).start()
    source(0, 1).start()
    copy(0).start()
    scalars[1].start()
    for scalar in scalars:
        scalar.wait()
    m = pair_wavenumber(slot_ref)
    m_ref[...] = m
    lane = lane_iota()
    even = row_iota() % 2 == 0
    small = m < LANES
    zero = jnp.zeros((ROWS, LANES), F32)
    keep1 = lane + LANES >= m
    keep3 = lane + 3 * LANES >= jnp.where(even, m, 511 - m)
    keep_mix = lane >= jnp.where(small, m, 255 - m)
    for f in range(FIELDS):
        source(f, 0).wait()
        if f == 0:
            for i in range(1, AHEAD):
                copy(i).start()

        target = first_v if f == 0 else packed_v

        def pack_points(i, carry):
            for k in range(8):
                pack_point(i * 8 + k)
            return carry

        def pack_point(q):
            s = [[src_v[f, q, c, :, b * LANES:(b + 1) * LANES] for b in range(4)] for c in range(2)]
            first = jnp.where(even, s[0][0], down(s[1][0]))
            late = jnp.where(even, up(s[0][2]), s[1][2])
            target[q, 0] = jnp.where(keep1, jnp.where(even, s[0][1], down(s[1][1])), 0.0)
            target[q, 1] = jnp.where(even, s[0][2], down(s[1][2]))
            target[q, 2] = jnp.where(keep3, s[0][3], 0.0)
            target[q, 3] = jnp.where(keep3, s[1][3], 0.0)
            target[q, 4] = jnp.where(keep_mix, jnp.where(small, first, late), 0.0)

        lax.fori_loop(0, POINTS // 16, pack_points, 0)
        source(f, 1).wait()
        lax.fori_loop(POINTS // 16, POINTS // 8, pack_points, 0)
        for q in (0, POINTS - 1):
            for v in range(PACK):
                target[q, v] = zero

        def weigh(block, carry):
            rows = pl.ds(block * PB, PB)
            pltpu.make_async_copy(inv_hbm.at[1, rows], later_v.at[rows], inv_sem.at[BLOCKS + block]).wait()
            weights = [[weight_ref[0, r, block * PB + p] for p in range(PB)] for r in range(2)]

            def tile_row(qb, carry):
                for b in range(4):
                    low, top = e_v[0, qb, b], e_v[1, qb, b]
                    for p in range(PB):
                        tile = later_v[block * PB + p, qb, :, b * LANES:(b + 1) * LANES]
                        low = low + weights[0][p] * tile
                        top = top + weights[1][p] * tile
                    e_v[0, qb, b] = low
                    e_v[1, qb, b] = top
                return carry

            return lax.fori_loop(0, POINTS // ROWS, tile_row, carry, unroll=4)

        def solve_and_weigh(block, carry):
            rows = pl.ds(block * PB, PB)
            pltpu.make_async_copy(inv_hbm.at[0, rows], inv_v.at[rows], inv_sem.at[block]).wait()

            @pl.when(block + AHEAD < BLOCKS)
            def _():
                ahead = pl.ds((block + AHEAD) * PB, PB)
                pltpu.make_async_copy(inv_hbm.at[0, ahead], inv_v.at[ahead], inv_sem.at[block + AHEAD]).start()

            @pl.when(block == 2)
            def _():
                source(1, 0).start()
                source(1, 1).start()

            pltpu.make_async_copy(inv_hbm.at[1, rows], later_v.at[rows], inv_sem.at[BLOCKS + block]).start()
            solve_block(f, inv_v, first_v, block, small, odd_v, part_v)
            sums = list(carry)
            for p in range(PB):
                at = block * PB + p
                x = [part_v[f, at, v] for v in range(KEPT)]
                for r in range(2):
                    weight = weight_ref[0, r, at]
                    for v in range(KEPT):
                        sums[r * KEPT + v] = sums[r * KEPT + v] + weight * x[v]
            return tuple(sums)

        if f == 0:
            sums = lax.fori_loop(0, BLOCKS, solve_and_weigh, (zero,) * (2 * KEPT))
            for r in range(2):
                for v in range(PACK):
                    msg_ref[r * PACK + v] = sums[r * KEPT + v]
                msg_ref[2 * PACK + r] = sums[r * KEPT + PACK]
            continue
        for r in range(2):
            for qb in range(POINTS // ROWS):
                for b in range(4):
                    e_v[r, qb, b] = zero
        lax.fori_loop(0, BLOCKS, weigh, 0)

        def accumulate(qb, sums):
            sums = list(sums)
            for row in range(ROWS):
                x = [packed_v[qb * ROWS + row, v] for v in range(PACK)]
                for r in range(2):
                    e = [jnp.broadcast_to(e_v[r, qb, b, row:row + 1, :], (ROWS, LANES)) for b in range(4)]
                    e = [e[1], e[2], e[3], e[3], jnp.where(small, e[0], e[2])]
                    for v in range(PACK):
                        sums[r * PACK + v] = sums[r * PACK + v] + e[v] * x[v]
            return tuple(sums)

        sums = lax.fori_loop(0, POINTS // ROWS, accumulate, (zero,) * (2 * PACK))
        for i in range(2 * PACK):
            msg_ref[f * MESSAGE + i] = sums[i]
        for r in range(2):
            for b in range(4):
                msg_ref[f * MESSAGE + 2 * PACK + r, 2 * b:2 * b + 1, :] = e_v[r, 0, b, 0:1, :]
                msg_ref[f * MESSAGE + 2 * PACK + r, 2 * b + 1:2 * b + 2, :] = (
                    e_v[r, POINTS // ROWS - 1, b, ROWS - 1:ROWS, :]
                )


ANY = pl.BlockSpec(memory_space=pl.ANY)
INVERSE_V = pltpu.VMEM((POINTS, POINTS // ROWS, ROWS, 512), F32)
PACKED_V = pltpu.VMEM((POINTS, PACK, ROWS, LANES), F32)
MESSAGE_V = pltpu.VMEM((FIELDS * MESSAGE, ROWS, LANES), F32)
PART_V = pltpu.VMEM((FIELDS, POINTS, KEPT, ROWS, LANES), F32)
SENT_V = pltpu.VMEM((GROUPS, SENT, ROWS, LANES), F32)
IN_VMEM = pl.BlockSpec(memory_space=pltpu.VMEM)
IN_HBM = pl.BlockSpec(memory_space=pltpu.HBM)


def grant(mib):
    return pltpu.CompilerParams(vmem_limit_bytes=mib * 2**20)


def held(x):
    return pltpu.with_memory_space_constraint(x, pltpu.VMEM)


def far(x):
    return pltpu.with_memory_space_constraint(x, pltpu.HBM)


def dma(*shape):
    return pltpu.SemaphoreType.DMA(shape)


def slopes(slot, weights, inverse, forcing):
    return pl.pallas_call(
        slope_kernel,
        in_specs=[IN_HBM] * 4,
        out_specs=[IN_VMEM] * 5,
        out_shape=[INVERSE_V, PACKED_V, MESSAGE_V, PART_V, pltpu.VMEM((ROWS, LANES), jnp.int32)],
        scratch_shapes=[
            INVERSE_V,
            pltpu.VMEM((FIELDS, POINTS, 2, ROWS, 512), F32),
            PACKED_V,
            pltpu.VMEM((2, POINTS // ROWS, 4, ROWS, LANES), F32),
            pltpu.VMEM((3 * PB, ROWS, LANES), F32),
            pltpu.SMEM((ROWS,), jnp.int32),
            pltpu.SMEM((1, 2, POINTS), F32),
            dma(CHUNKS),
            dma(2 * FIELDS),
            dma(2),
        ],
        compiler_params=grant(SLOPES_MIB),
        cost_estimate=pl.CostEstimate(flops=20_000_000, bytes_accessed=24_000_000, transcendentals=0),
        name="slopes",
    )(far(slot), far(weights), far(inverse), far(forcing))


def block_sums(f, inv_v, packed_v, block, small, odd_v):
    zero = jnp.zeros((ROWS, LANES), F32)

    def unit(p, qb, r, b):
        line = inv_v[block * PB + p, qb, r:r + 1, b * LANES:(b + 1) * LANES]
        return jnp.broadcast_to(line, (ROWS, LANES))

    def odd_rows(qb, sums, rows):
        sums = list(sums)
        for r in rows:
            s = [packed_v[qb * ROWS + r, v] for v in (0, 2, 3)]
            for p in range(PB):
                one = unit(p, qb, r, 1)
                three = unit(p, qb, r, 3)
                sums[3 * p] = sums[3 * p] + one * s[0]
                sums[3 * p + 1] = sums[3 * p + 1] + three * s[1]
                sums[3 * p + 2] = sums[3 * p + 2] + three * s[2]
        return tuple(sums)

    def even_rows(qb, sums, rows):
        sums = list(sums)
        for r in rows:
            s = [packed_v[qb * ROWS + r, v] for v in (1, 4)]
            for p in range(PB):
                none = unit(p, qb, r, 0)
                two = unit(p, qb, r, 2)
                sums[2 * p] = sums[2 * p] + two * s[0]
                sums[2 * p + 1] = sums[2 * p + 1] + jnp.where(small, none, two) * s[1]
        return tuple(sums)

    def all_rows(rows_of, sums):
        last = POINTS // ROWS - 1
        sums = rows_of(0, sums, range(1, ROWS))
        sums = lax.fori_loop(1, last, lambda qb, c: rows_of(qb, c, range(ROWS)), sums, unroll=2)
        return rows_of(last, sums, range(ROWS - 1))

    odd = all_rows(odd_rows, (zero,) * (3 * PB))
    for i in range(3 * PB):
        odd_v[i] = odd[i]
    even = all_rows(even_rows, (zero,) * (2 * PB))
    return [[odd_v[3 * p], even[2 * p], odd_v[3 * p + 1], odd_v[3 * p + 2], even[2 * p + 1]] for p in range(PB)]


def solve_block(f, inv_v, packed_v, block, small, odd_v, part_v):
    x = block_sums(f, inv_v, packed_v, block, small, odd_v)
    for p in range(PB):
        at = block * PB + p
        for v in range(PACK):
            part_v[f, at, v] = x[p][v]
        for b in range(4):
            lanes = slice(b * LANES, (b + 1) * LANES)
            part_v[f, at, PACK, 2 * b:2 * b + 1, :] = inv_v[at, 0, 0:1, lanes]
            part_v[f, at, PACK, 2 * b + 1:2 * b + 2, :] = inv_v[at, POINTS // ROWS - 1, ROWS - 1:ROWS, lanes]


def particular_kernel(m_ref, inv_v, packed_v, early_v, part_v, odd_v):
    small = m_ref[...] < LANES

    def step(block, carry):
        solve_block(FIELDS - 1, inv_v, packed_v, block, small, odd_v, part_v)
        return carry

    lax.fori_loop(0, BLOCKS, step, 0)


def particular(m, inverse, packed, early):
    return pl.pallas_call(
        particular_kernel,
        in_specs=[IN_VMEM] * 4,
        out_specs=IN_VMEM,
        out_shape=PART_V,
        input_output_aliases={3: 0},
        scratch_shapes=[pltpu.VMEM((3 * PB, ROWS, LANES), F32)],
        compiler_params=grant(PARTICULAR_MIB),
        cost_estimate=pl.CostEstimate(flops=90_000_000, bytes_accessed=24_000_000, transcendentals=0),
        name="particular",
    )(held(m), held(inverse), held(packed), held(early))


def solve_interface(f, all_v, u_v, small):
    base = f * MESSAGE
    zero = jnp.zeros((ROWS, LANES), F32)
    for v in range(PACK):
        u_v[0, f, v] = zero
        u_v[NSUB, f, v] = zero

    def coefficient(t, r, k, b):
        return all_v[t, base + 2 * PACK + r, pl.ds(2 * b + k, ROWS, stride=0), :]

    ratio = [zero] * PACK
    reduced = [zero] * PACK
    ratios = []
    reduceds = []
    for level in range(NSUB - 1):
        factors = []
        for b in range(4):
            lower = coefficient(level, 1, 0, b)
            middle = coefficient(level, 1, 1, b) - coefficient(level + 1, 0, 0, b)
            upper = -coefficient(level + 1, 0, 1, b)
            factors.append((lower, middle, upper))
        mixed = tuple(jnp.where(small, x, y) for x, y in zip(factors[0], factors[2]))
        new_ratio, new_reduced = [None] * PACK, [None] * PACK
        for v, (lower, middle, upper) in enumerate((factors[1], factors[2], factors[3], factors[3], mixed)):
            right = all_v[level + 1, base + v] - all_v[level, base + PACK + v]
            inverted = last if v == 3 else 1.0 / (middle - lower * ratio[v])
            last = inverted
            new_ratio[v] = upper * inverted
            new_reduced[v] = (right - lower * reduced[v]) * inverted
        ratio, reduced = new_ratio, new_reduced
        ratios.append(ratio)
        reduceds.append(reduced)
    later = [zero] * PACK
    for level in range(NSUB - 2, -1, -1):
        later = [reduceds[level][v] - ratios[level][v] * later[v] for v in range(PACK)]
        for v in range(PACK):
            u_v[level + 1, f, v] = later[v]


PER = PB // NEAR


def pack_kernel(m_ref, *refs):
    blocks = refs[:NSUB]
    part_v, out_v, all_v, u_v = refs[NSUB:]
    sub = lax.axis_index("sub")
    level, core = sub // 2, lax.rem(sub, 2)
    for k in range(NSUB):
        other, turn = k // 4, k % 4
        place = lax.rem(level + (4 - turn), 4) * 2 + (core if other == 0 else 1 - core)
        for i in range(FIELDS * MESSAGE):
            all_v[place, i] = blocks[k][i]
    m = m_ref[...]
    lane = lane_iota()
    even = row_iota() % 2 == 0
    small = m < LANES
    for f in range(FIELDS):
        solve_interface(f, all_v, u_v, small)

    def step(block, carry):
        for d in range(PER):
            dest = block * PER + d
            extra = jnp.where(lane == FIELDS * NEAR, m.astype(F32), 0.0)
            for f in range(FIELDS):
                u_low = [u_v[sub, f, v] for v in range(PACK)]
                u_top = [u_v[sub + 1, f, v] for v in range(PACK)]
                for k in range(NEAR):
                    p = block * PB + d * NEAR + k
                    low = [part_v[f, p, PACK, pl.ds(2 * b, ROWS, stride=0), :] for b in range(4)]
                    top = [part_v[f, p, PACK, pl.ds(2 * b + 1, ROWS, stride=0), :] for b in range(4)]
                    low = [low[1], low[2], low[3], low[3], jnp.where(small, low[0], low[2])]
                    top = [top[1], top[2], top[3], top[3], jnp.where(small, top[0], top[2])]
                    x = [part_v[f, p, v] + u_low[v] * low[v] + u_top[v] * top[v] for v in range(PACK)]
                    s, spare = fold(x, m, lane, even, small)
                    at = f * NEAR + k
                    for b in range(4):
                        out_v[dest, at * 4 + b] = s[b]
                    extra = jnp.where(lane == at, spare, extra)
            out_v[dest, SENT - 1] = extra
        return carry

    lax.fori_loop(0, BLOCKS, step, 0)


def pack(m, messages, part):
    return pl.pallas_call(
        pack_kernel,
        in_specs=[IN_VMEM] * (NSUB + 2),
        out_specs=IN_VMEM,
        out_shape=SENT_V,
        scratch_shapes=[
            pltpu.VMEM((NSUB, FIELDS * MESSAGE, ROWS, LANES), F32),
            pltpu.VMEM((NSUB + 1, FIELDS, PACK, ROWS, LANES), F32),
        ],
        compiler_params=grant(PACK_MIB),
        name="pack",
    )(held(m), *[held(x) for x in messages], held(part))


STEPS = 8
FROM = GROUPS // STEPS


def unpack_kernel(in_v, out_hbm, out_v, out_sem):
    def out_copy(i):
        rows = pl.ds(pl.multiple_of(i * FROM * ROWS, ROWS), FROM * ROWS)
        return pltpu.make_async_copy(out_v.at[:, :, :, rows, :], out_hbm.at[:, :, :, rows, :], out_sem.at[i])

    lane = lane_iota()
    even = row_iota() % 2 == 0

    def step(i, carry):
        for d in range(FROM):
            g = i * FROM + d
            extras = in_v[g, SENT - 1]
            m = column(extras, FIELDS * NEAR).astype(jnp.int32)
            small = m < LANES
            rows = pl.ds(pl.multiple_of(g * ROWS, ROWS), ROWS)
            for f in range(FIELDS):
                for k in range(NEAR):
                    at = f * NEAR + k
                    s = [in_v[g, at * 4 + b] for b in range(4)]
                    tiles = unfold(s, column(extras, at), m, lane, even, small)
                    for c in range(2):
                        for b in range(4):
                            out_v[f, k, c, rows, b * LANES:(b + 1) * LANES] = tiles[c][b]
        out_copy(i).start()
        return carry

    lax.fori_loop(0, STEPS, step, 0)
    wait_all(out_copy, STEPS)


def unpack(received):
    return pl.pallas_call(
        unpack_kernel,
        in_specs=[IN_VMEM],
        out_specs=ANY,
        out_shape=jax.ShapeDtypeStruct((FIELDS, NEAR, 2, GROUPS * ROWS, 512), F32),
        scratch_shapes=[pltpu.VMEM((FIELDS, NEAR, 2, GROUPS * ROWS, 512), F32), dma(STEPS)],
        compiler_params=grant(UNPACK_MIB),
        name="unpack",
    )(held(received))


def over_ma(sent):
    flat = sent.reshape(GROUPS, SENT * ROWS, LANES)
    received = lax.all_to_all(flat, "ma", split_axis=0, concat_axis=0, tiled=True)
    return received.reshape(GROUPS, SENT, ROWS, LANES)


def body(forcing, slot_wavenumber, inverse, edge_weights):
    inverse = inverse.reshape(FIELDS, POINTS, POINTS // ROWS, ROWS, 512)
    later, packed, message, early, m = slopes(slot_wavenumber, edge_weights, inverse, forcing)
    column = [message]
    for k in range(1, 4):
        column.append(lax.ppermute(message, "sub", [(i, (i + 2 * k) % NSUB) for i in range(NSUB)]))
    part = particular(m, later, packed, early)
    partner = [(i, i ^ 1) for i in range(NSUB)]
    twin = [lax.ppermute(message, "sub", partner)]
    part, *column[1:] = lax.optimization_barrier((part, *column[1:]))
    messages = column + twin + [lax.ppermute(x, "sub", partner) for x in column[1:]]
    sent = pack(m, messages, part)
    return unpack(over_ma(sent))


def solution(mesh):
    return jax.shard_map(
        body,
        mesh=mesh,
        in_specs=(
            P(None, "sub", None, "ma", None),
            P("ma"),
            P("sub", None, None, None, None),
            P("sub", None, None),
        ),
        out_specs=P(None, ("sub", "ma"), None, None, None),
        check_vma=False,
    )
```

```python
import jax
import jax.numpy as jnp
from jax import lax
from jax.experimental import pallas as pl
from jax.experimental.pallas import tpu as pltpu
from jax.sharding import PartitionSpec as P

F32 = jnp.float32
POINTS = 64
FIELDS = 2
NSUB = 8
GROUPS = 16
LANES = 128
ROWS = 8
PACK = 5
QB = 8
PB = 8
NEAR = POINTS // GROUPS
SENT = FIELDS * NEAR * 4 + 1
MESSAGE = 2 * PACK + 2
BLOCKS = POINTS // PB


def lane_iota():
    return lax.broadcasted_iota(jnp.int32, (ROWS, LANES), 1)


def row_iota():
    return lax.broadcasted_iota(jnp.int32, (ROWS, LANES), 0)


def pair_wavenumber(slot_ref):
    pair = row_iota() // 2
    m = jnp.full((ROWS, LANES), slot_ref[0], jnp.int32)
    for j in range(1, 4):
        m = jnp.where(pair == j, slot_ref[2 * j], m)
    return m


def down(x):
    return pltpu.roll(x, 1, 0)


def up(x):
    return pltpu.roll(x, ROWS - 1, 0)


def fold(x, m, lane, even, small):
    shift = jnp.where(small, m, m - LANES)
    turn = (lane - shift + LANES) % LANES
    below = lane < shift
    low3 = jnp.where(even, x[2], down(x[3]))
    high3 = jnp.where(even, up(x[2]), x[3])
    high3_t = jnp.take_along_axis(high3, turn, axis=1)
    mix_t = jnp.take_along_axis(x[4], turn, axis=1)
    zero = jnp.where(small, jnp.where(below, high3_t, x[4]), jnp.where(below, mix_t, high3_t))
    one = jnp.where(jnp.logical_and(below, jnp.logical_not(small)), high3_t, x[0])
    last = jnp.full((ROWS, LANES), LANES - 1, jnp.int32)
    spare = jnp.take_along_axis(jnp.where(small, high3_t, mix_t), last, axis=1)
    return (zero, one, x[1], low3), spare


def column(x, k):
    return jnp.take_along_axis(x, jnp.full((ROWS, LANES), k, jnp.int32), axis=1)


def unfold(s, spare, m, lane, even, small):
    shift = jnp.where(small, m, m - LANES)
    back = (lane + shift) % LANES
    after = lane >= LANES - shift
    exact = lane == LANES - 1 - shift
    g0 = jnp.take_along_axis(s[0], back, axis=1)
    g1 = jnp.take_along_axis(s[1], back, axis=1)
    value = jnp.where(after, g0, jnp.where(exact, spare, 0.0))
    high3 = jnp.where(small, value, jnp.where(after, g1, g0))
    high2 = jnp.where(small, 0.0, value)
    low0 = jnp.where(lane >= m, s[0], 0.0)
    low1 = jnp.where(lane + LANES >= m, s[1], 0.0)
    lows = [low0, low1, s[2], s[3]]
    first = [jnp.where(even, low0, 0.0), jnp.where(even, low1, 0.0)]
    first += [jnp.where(even, s[2], down(high2)), jnp.where(even, s[3], down(high3))]
    second = [jnp.where(even, up(low0), 0.0), jnp.where(even, up(low1), 0.0)]
    second += [jnp.where(even, up(s[2]), high2), jnp.where(even, up(s[3]), high3)]
    return first, second


AHEAD = 3
SLOPES_MIB = 18
PARTICULAR_MIB = 4
PACK_MIB = 4
UNPACK_MIB = 8
KEPT = PACK + 1
CHUNKS = FIELDS * BLOCKS


def inverse_chunks(inv_hbm, held_v, sem):
    def copy(i):
        f, block = i // BLOCKS, i % BLOCKS
        rows = pl.ds(block * PB, PB)
        return pltpu.make_async_copy(inv_hbm.at[f, rows], held_v[f].at[rows], sem.at[i])

    return copy


def wait_all(copy, count, first=0):
    def step(i, carry):
        copy(i).wait()
        return carry

    lax.fori_loop(first, count, step, 0)


def slope_kernel(
    slot_hbm, weight_hbm, inv_hbm, src_hbm, later_v, packed_v, msg_ref, part_v, m_ref,
    inv_v, src_v, first_v, e_v, odd_v, slot_ref, weight_ref, inv_sem, src_sem, scalar_sem
):
    copy = inverse_chunks(inv_hbm, (inv_v, later_v), inv_sem)
    def source(f, half):
        rows = pl.ds(half * (POINTS // 2), POINTS // 2)
        return pltpu.make_async_copy(src_hbm.at[f, rows], src_v.at[f, rows], src_sem.at[2 * f + half])


    scalars = [
        pltpu.make_async_copy(slot_hbm, slot_ref, scalar_sem.at[0]),
        pltpu.make_async_copy(weight_hbm, weight_ref, scalar_sem.at[1]),
    ]
    scalars[0].start()
    source(0, 0).start()
    source(0, 1).start()
    copy(0).start()
    scalars[1].start()
    for scalar in scalars:
        scalar.wait()
    m = pair_wavenumber(slot_ref)
    m_ref[...] = m
    lane = lane_iota()
    even = row_iota() % 2 == 0
    small = m < LANES
    zero = jnp.zeros((ROWS, LANES), F32)
    keep1 = lane + LANES >= m
    keep3 = lane + 3 * LANES >= jnp.where(even, m, 511 - m)
    keep_mix = lane >= jnp.where(small, m, 255 - m)
    for f in range(FIELDS):
        source(f, 0).wait()
        if f == 0:
            for i in range(1, AHEAD):
                copy(i).start()

        target = first_v if f == 0 else packed_v

        def pack_points(i, carry):
            for k in range(8):
                pack_point(i * 8 + k)
            return carry

        def pack_point(q):
            s = [[src_v[f, q, c, :, b * LANES:(b + 1) * LANES] for b in range(4)] for c in range(2)]
            first = jnp.where(even, s[0][0], down(s[1][0]))
            late = jnp.where(even, up(s[0][2]), s[1][2])
            target[q, 0] = jnp.where(keep1, jnp.where(even, s[0][1], down(s[1][1])), 0.0)
            target[q, 1] = jnp.where(even, s[0][2], down(s[1][2]))
            target[q, 2] = jnp.where(keep3, s[0][3], 0.0)
            target[q, 3] = jnp.where(keep3, s[1][3], 0.0)
            target[q, 4] = jnp.where(keep_mix, jnp.where(small, first, late), 0.0)

        lax.fori_loop(0, POINTS // 16, pack_points, 0)
        source(f, 1).wait()
        lax.fori_loop(POINTS // 16, POINTS // 8, pack_points, 0)
        for q in (0, POINTS - 1):
            for v in range(PACK):
                target[q, v] = zero

        def weigh(block, carry):
            rows = pl.ds(block * PB, PB)
            pltpu.make_async_copy(inv_hbm.at[1, rows], later_v.at[rows], inv_sem.at[BLOCKS + block]).wait()
            weights = [[weight_ref[0, r, block * PB + p] for p in range(PB)] for r in range(2)]

            def tile_row(qb, carry):
                for b in range(4):
                    low, top = e_v[0, qb, b], e_v[1, qb, b]
                    for p in range(PB):
                        tile = later_v[block * PB + p, qb, :, b * LANES:(b + 1) * LANES]
                        low = low + weights[0][p] * tile
                        top = top + weights[1][p] * tile
                    e_v[0, qb, b] = low
                    e_v[1, qb, b] = top
                return carry

            return lax.fori_loop(0, POINTS // ROWS, tile_row, carry, unroll=4)

        def solve_and_weigh(block, carry):
            rows = pl.ds(block * PB, PB)
            pltpu.make_async_copy(inv_hbm.at[0, rows], inv_v.at[rows], inv_sem.at[block]).wait()

            @pl.when(block + AHEAD < BLOCKS)
            def _():
                ahead = pl.ds((block + AHEAD) * PB, PB)
                pltpu.make_async_copy(inv_hbm.at[0, ahead], inv_v.at[ahead], inv_sem.at[block + AHEAD]).start()

            @pl.when(block == 2)
            def _():
                source(1, 0).start()
                source(1, 1).start()

            pltpu.make_async_copy(inv_hbm.at[1, rows], later_v.at[rows], inv_sem.at[BLOCKS + block]).start()
            solve_block(f, inv_v, first_v, block, small, odd_v, part_v)
            sums = list(carry)
            for p in range(PB):
                at = block * PB + p
                x = [part_v[f, at, v] for v in range(KEPT)]
                for r in range(2):
                    weight = weight_ref[0, r, at]
                    for v in range(KEPT):
                        sums[r * KEPT + v] = sums[r * KEPT + v] + weight * x[v]
            return tuple(sums)

        if f == 0:
            sums = lax.fori_loop(0, BLOCKS, solve_and_weigh, (zero,) * (2 * KEPT))
            for r in range(2):
                for v in range(PACK):
                    msg_ref[r * PACK + v] = sums[r * KEPT + v]
                msg_ref[2 * PACK + r] = sums[r * KEPT + PACK]
            continue
        for r in range(2):
            for qb in range(POINTS // ROWS):
                for b in range(4):
                    e_v[r, qb, b] = zero
        lax.fori_loop(0, BLOCKS, weigh, 0)

        def accumulate(qb, sums):
            sums = list(sums)
            for row in range(ROWS):
                x = [packed_v[qb * ROWS + row, v] for v in range(PACK)]
                for r in range(2):
                    e = [jnp.broadcast_to(e_v[r, qb, b, row:row + 1, :], (ROWS, LANES)) for b in range(4)]
                    e = [e[1], e[2], e[3], e[3], jnp.where(small, e[0], e[2])]
                    for v in range(PACK):
                        sums[r * PACK + v] = sums[r * PACK + v] + e[v] * x[v]
            return tuple(sums)

        sums = lax.fori_loop(0, POINTS // ROWS, accumulate, (zero,) * (2 * PACK))
        for i in range(2 * PACK):
            msg_ref[f * MESSAGE + i] = sums[i]
        for r in range(2):
            for b in range(4):
                msg_ref[f * MESSAGE + 2 * PACK + r, 2 * b:2 * b + 1, :] = e_v[r, 0, b, 0:1, :]
                msg_ref[f * MESSAGE + 2 * PACK + r, 2 * b + 1:2 * b + 2, :] = (
                    e_v[r, POINTS // ROWS - 1, b, ROWS - 1:ROWS, :]
                )


ANY = pl.BlockSpec(memory_space=pl.ANY)
INVERSE_V = pltpu.VMEM((POINTS, POINTS // ROWS, ROWS, 512), F32)
PACKED_V = pltpu.VMEM((POINTS, PACK, ROWS, LANES), F32)
MESSAGE_V = pltpu.VMEM((FIELDS * MESSAGE, ROWS, LANES), F32)
PART_V = pltpu.VMEM((FIELDS, POINTS, KEPT, ROWS, LANES), F32)
SENT_V = pltpu.VMEM((GROUPS, SENT, ROWS, LANES), F32)
IN_VMEM = pl.BlockSpec(memory_space=pltpu.VMEM)
IN_HBM = pl.BlockSpec(memory_space=pltpu.HBM)


def grant(mib):
    return pltpu.CompilerParams(vmem_limit_bytes=mib * 2**20)


def held(x):
    return pltpu.with_memory_space_constraint(x, pltpu.VMEM)


def far(x):
    return pltpu.with_memory_space_constraint(x, pltpu.HBM)


def dma(*shape):
    return pltpu.SemaphoreType.DMA(shape)


def slopes(slot, weights, inverse, forcing):
    return pl.pallas_call(
        slope_kernel,
        in_specs=[IN_HBM] * 4,
        out_specs=[IN_VMEM] * 5,
        out_shape=[INVERSE_V, PACKED_V, MESSAGE_V, PART_V, pltpu.VMEM((ROWS, LANES), jnp.int32)],
        scratch_shapes=[
            INVERSE_V,
            pltpu.VMEM((FIELDS, POINTS, 2, ROWS, 512), F32),
            PACKED_V,
            pltpu.VMEM((2, POINTS // ROWS, 4, ROWS, LANES), F32),
            pltpu.VMEM((3 * PB, ROWS, LANES), F32),
            pltpu.SMEM((ROWS,), jnp.int32),
            pltpu.SMEM((1, 2, POINTS), F32),
            dma(CHUNKS),
            dma(2 * FIELDS),
            dma(2),
        ],
        compiler_params=grant(SLOPES_MIB),
        cost_estimate=pl.CostEstimate(flops=20_000_000, bytes_accessed=24_000_000, transcendentals=0),
        name="slopes",
    )(far(slot), far(weights), far(inverse), far(forcing))


def block_sums(f, inv_v, packed_v, block, small, odd_v):
    zero = jnp.zeros((ROWS, LANES), F32)

    def unit(p, qb, r, b):
        line = inv_v[block * PB + p, qb, r:r + 1, b * LANES:(b + 1) * LANES]
        return jnp.broadcast_to(line, (ROWS, LANES))

    def odd_rows(qb, sums, rows):
        sums = list(sums)
        for r in rows:
            s = [packed_v[qb * ROWS + r, v] for v in (0, 2, 3)]
            for p in range(PB):
                one = unit(p, qb, r, 1)
                three = unit(p, qb, r, 3)
                sums[3 * p] = sums[3 * p] + one * s[0]
                sums[3 * p + 1] = sums[3 * p + 1] + three * s[1]
                sums[3 * p + 2] = sums[3 * p + 2] + three * s[2]
        return tuple(sums)

    def even_rows(qb, sums, rows):
        sums = list(sums)
        for r in rows:
            s = [packed_v[qb * ROWS + r, v] for v in (1, 4)]
            for p in range(PB):
                none = unit(p, qb, r, 0)
                two = unit(p, qb, r, 2)
                sums[2 * p] = sums[2 * p] + two * s[0]
                sums[2 * p + 1] = sums[2 * p + 1] + jnp.where(small, none, two) * s[1]
        return tuple(sums)

    def all_rows(rows_of, sums):
        last = POINTS // ROWS - 1
        sums = rows_of(0, sums, range(1, ROWS))
        sums = lax.fori_loop(1, last, lambda qb, c: rows_of(qb, c, range(ROWS)), sums, unroll=2)
        return rows_of(last, sums, range(ROWS - 1))

    odd = all_rows(odd_rows, (zero,) * (3 * PB))
    for i in range(3 * PB):
        odd_v[i] = odd[i]
    even = all_rows(even_rows, (zero,) * (2 * PB))
    return [[odd_v[3 * p], even[2 * p], odd_v[3 * p + 1], odd_v[3 * p + 2], even[2 * p + 1]] for p in range(PB)]


def solve_block(f, inv_v, packed_v, block, small, odd_v, part_v):
    x = block_sums(f, inv_v, packed_v, block, small, odd_v)
    for p in range(PB):
        at = block * PB + p
        for v in range(PACK):
            part_v[f, at, v] = x[p][v]
        for b in range(4):
            lanes = slice(b * LANES, (b + 1) * LANES)
            part_v[f, at, PACK, 2 * b:2 * b + 1, :] = inv_v[at, 0, 0:1, lanes]
            part_v[f, at, PACK, 2 * b + 1:2 * b + 2, :] = inv_v[at, POINTS // ROWS - 1, ROWS - 1:ROWS, lanes]


def particular_kernel(m_ref, inv_v, packed_v, early_v, part_v, odd_v):
    small = m_ref[...] < LANES

    def step(block, carry):
        solve_block(FIELDS - 1, inv_v, packed_v, block, small, odd_v, part_v)
        return carry

    lax.fori_loop(0, BLOCKS, step, 0)


def particular(m, inverse, packed, early):
    return pl.pallas_call(
        particular_kernel,
        in_specs=[IN_VMEM] * 4,
        out_specs=IN_VMEM,
        out_shape=PART_V,
        input_output_aliases={3: 0},
        scratch_shapes=[pltpu.VMEM((3 * PB, ROWS, LANES), F32)],
        compiler_params=grant(PARTICULAR_MIB),
        cost_estimate=pl.CostEstimate(flops=90_000_000, bytes_accessed=24_000_000, transcendentals=0),
        name="particular",
    )(held(m), held(inverse), held(packed), held(early))


def solve_interface(f, all_v, u_v, small):
    base = f * MESSAGE
    zero = jnp.zeros((ROWS, LANES), F32)
    for v in range(PACK):
        u_v[0, f, v] = zero
        u_v[NSUB, f, v] = zero

    def coefficient(t, r, k, b):
        return all_v[t, base + 2 * PACK + r, pl.ds(2 * b + k, ROWS, stride=0), :]

    ratio = [zero] * PACK
    reduced = [zero] * PACK
    ratios = []
    reduceds = []
    for level in range(NSUB - 1):
        factors = []
        for b in range(4):
            lower = coefficient(level, 1, 0, b)
            middle = coefficient(level, 1, 1, b) - coefficient(level + 1, 0, 0, b)
            upper = -coefficient(level + 1, 0, 1, b)
            factors.append((lower, middle, upper))
        mixed = tuple(jnp.where(small, x, y) for x, y in zip(factors[0], factors[2]))
        new_ratio, new_reduced = [None] * PACK, [None] * PACK
        for v, (lower, middle, upper) in enumerate((factors[1], factors[2], factors[3], factors[3], mixed)):
            right = all_v[level + 1, base + v] - all_v[level, base + PACK + v]
            inverted = last if v == 3 else 1.0 / (middle - lower * ratio[v])
            last = inverted
            new_ratio[v] = upper * inverted
            new_reduced[v] = (right - lower * reduced[v]) * inverted
        ratio, reduced = new_ratio, new_reduced
        ratios.append(ratio)
        reduceds.append(reduced)
    later = [zero] * PACK
    for level in range(NSUB - 2, -1, -1):
        later = [reduceds[level][v] - ratios[level][v] * later[v] for v in range(PACK)]
        for v in range(PACK):
            u_v[level + 1, f, v] = later[v]


PER = PB // NEAR


def pack_kernel(m_ref, *refs):
    blocks = refs[:NSUB]
    part_v, out_v, all_v, u_v = refs[NSUB:]
    sub = lax.axis_index("sub")
    level, core = sub // 2, lax.rem(sub, 2)
    for k in range(NSUB):
        other, turn = k // 4, k % 4
        place = lax.rem(level + (4 - turn), 4) * 2 + (core if other == 0 else 1 - core)
        for i in range(FIELDS * MESSAGE):
            all_v[place, i] = blocks[k][i]
    m = m_ref[...]
    lane = lane_iota()
    even = row_iota() % 2 == 0
    small = m < LANES
    for f in range(FIELDS):
        solve_interface(f, all_v, u_v, small)

    def step(block, carry):
        for d in range(PER):
            dest = block * PER + d
            extra = jnp.where(lane == FIELDS * NEAR, m.astype(F32), 0.0)
            for f in range(FIELDS):
                u_low = [u_v[sub, f, v] for v in range(PACK)]
                u_top = [u_v[sub + 1, f, v] for v in range(PACK)]
                for k in range(NEAR):
                    p = block * PB + d * NEAR + k
                    low = [part_v[f, p, PACK, pl.ds(2 * b, ROWS, stride=0), :] for b in range(4)]
                    top = [part_v[f, p, PACK, pl.ds(2 * b + 1, ROWS, stride=0), :] for b in range(4)]
                    low = [low[1], low[2], low[3], low[3], jnp.where(small, low[0], low[2])]
                    top = [top[1], top[2], top[3], top[3], jnp.where(small, top[0], top[2])]
                    x = [part_v[f, p, v] + u_low[v] * low[v] + u_top[v] * top[v] for v in range(PACK)]
                    s, spare = fold(x, m, lane, even, small)
                    at = f * NEAR + k
                    for b in range(4):
                        out_v[dest, at * 4 + b] = s[b]
                    extra = jnp.where(lane == at, spare, extra)
            out_v[dest, SENT - 1] = extra
        return carry

    lax.fori_loop(0, BLOCKS, step, 0, unroll=2)


def pack(m, messages, part):
    return pl.pallas_call(
        pack_kernel,
        in_specs=[IN_VMEM] * (NSUB + 2),
        out_specs=IN_VMEM,
        out_shape=SENT_V,
        scratch_shapes=[
            pltpu.VMEM((NSUB, FIELDS * MESSAGE, ROWS, LANES), F32),
            pltpu.VMEM((NSUB + 1, FIELDS, PACK, ROWS, LANES), F32),
        ],
        compiler_params=grant(PACK_MIB),
        name="pack",
    )(held(m), *[held(x) for x in messages], held(part))


STEPS = 4
FROM = GROUPS // STEPS


def unpack_kernel(in_v, out_hbm, out_v, out_sem):
    def out_copy(i):
        rows = pl.ds(pl.multiple_of(i * FROM * ROWS, ROWS), FROM * ROWS)
        return pltpu.make_async_copy(out_v.at[:, :, :, rows, :], out_hbm.at[:, :, :, rows, :], out_sem.at[i])

    lane = lane_iota()
    even = row_iota() % 2 == 0

    def step(i, carry):
        for d in range(FROM):
            g = i * FROM + d
            extras = in_v[g, SENT - 1]
            m = column(extras, FIELDS * NEAR).astype(jnp.int32)
            small = m < LANES
            rows = pl.ds(pl.multiple_of(g * ROWS, ROWS), ROWS)
            for f in range(FIELDS):
                for k in range(NEAR):
                    at = f * NEAR + k
                    s = [in_v[g, at * 4 + b] for b in range(4)]
                    tiles = unfold(s, column(extras, at), m, lane, even, small)
                    for c in range(2):
                        for b in range(4):
                            out_v[f, k, c, rows, b * LANES:(b + 1) * LANES] = tiles[c][b]
        out_copy(i).start()
        return carry

    lax.fori_loop(0, STEPS, step, 0)
    wait_all(out_copy, STEPS)


def unpack(received):
    return pl.pallas_call(
        unpack_kernel,
        in_specs=[IN_VMEM],
        out_specs=ANY,
        out_shape=jax.ShapeDtypeStruct((FIELDS, NEAR, 2, GROUPS * ROWS, 512), F32),
        scratch_shapes=[pltpu.VMEM((FIELDS, NEAR, 2, GROUPS * ROWS, 512), F32), dma(STEPS)],
        compiler_params=grant(UNPACK_MIB),
        name="unpack",
    )(held(received))


def over_ma(sent):
    flat = sent.reshape(GROUPS, SENT * ROWS, LANES)
    received = lax.all_to_all(flat, "ma", split_axis=0, concat_axis=0, tiled=True)
    return received.reshape(GROUPS, SENT, ROWS, LANES)


def body(forcing, slot_wavenumber, inverse, edge_weights):
    inverse = inverse.reshape(FIELDS, POINTS, POINTS // ROWS, ROWS, 512)
    later, packed, message, early, m = slopes(slot_wavenumber, edge_weights, inverse, forcing)
    column = [message]
    for k in range(1, 4):
        column.append(lax.ppermute(message, "sub", [(i, (i + 2 * k) % NSUB) for i in range(NSUB)]))
    part = particular(m, later, packed, early)
    partner = [(i, i ^ 1) for i in range(NSUB)]
    twin = [lax.ppermute(message, "sub", partner)]
    part, *column[1:] = lax.optimization_barrier((part, *column[1:]))
    messages = column + twin + [lax.ppermute(x, "sub", partner) for x in column[1:]]
    sent = pack(m, messages, part)
    return unpack(over_ma(sent))


def solution(mesh):
    return jax.shard_map(
        body,
        mesh=mesh,
        in_specs=(
            P(None, "sub", None, "ma", None),
            P("ma"),
            P("sub", None, None, None, None),
            P("sub", None, None),
        ),
        out_specs=P(None, ("sub", "ma"), None, None, None),
        check_vma=False,
    )
```
